32 devices in a mesh: section: 2 (over core), mp: 4 (over y, x), dp: 4 (over z).
Axes of the slice: x: 2, y: 2, z: 4, core: 2. Of those that a mesh axis runs over, the one named last changes fastest.
Arguments:
- value_grad: bfloat16 [2, 2048, 3072], P('section', 'dp', 'mp'), may hold values from -6 to 6
- stream: bfloat16 [2, 2048, 3072], P('section', 'dp'), may hold values from -300 to 300
- weights: bfloat16 [2, 3072, 3072], P('section', 'mp'), may hold values from -0.109375 to 0.109375
- gain: float32 [2, 3072], P('section'), may hold values from 0.25 to 1.75
- top_grad: bfloat16 [2048, 3072], P('dp'), may hold values from -6 to 6
- counts: int32 [4], P('dp'), may hold values from 1 to 2, as said below
Outputs:
- weight_grad: bfloat16 [2, 3072, 3072], P('section', ('mp', 'dp'))
- residual_grad: bfloat16 [2, 2048, 3072], P('section', 'dp', 'mp')
The draws below stay inside these ranges and needn't reach their ends.
Inputs may be any that keep to these rules, and one draw needn't show every extreme that they name: counts[r] counts the live micro-batches of replica r; some replica has all 2.
All inputs are finite; a program needn't handle non-finite values.
Results may differ from the reference program's by a relative error of at most 0.009.
Values may be sent and summed in bfloat16 or wider, within the bound.
A program may use at most 64 MiB of HBM per device.

```python
import jax
import jax.numpy as jnp
from jax import lax

D = 3072
F = 3072
MICRO = 2
TOK_MB = 256
GROUPS = 4
REPLICAS = 4
TOKENS = 2048


def draw_stream(key, part):
    first, second, third = jax.random.split(key, 3)
    row_scale = jnp.exp(jax.random.uniform(second, (2, TOKENS, 1), jnp.float32) * jnp.log(10.0))
    col_scale = jnp.exp(jax.random.uniform(third, (2, 1, D), jnp.float32) * jnp.log(10.0))
    base = jax.random.normal(first, (2, TOKENS, D), jnp.float32)
    values = jnp.clip(base * row_scale * col_scale * 0.3, -300.0, 300.0)
    return values.astype(jnp.bfloat16)


def draw_counts(key, part):
    first, second = jax.random.split(jax.random.fold_in(key, 7))
    drawn = jax.random.randint(first, (REPLICAS,), 1, MICRO + 1)
    chosen = jax.random.randint(second, (), 0, REPLICAS)
    drawn = drawn.at[chosen].set(MICRO)
    return drawn.astype(jnp.int32)


def strengthened(entries, rng, source, target, shards_of, factor):
    def block_of(position):
        return (jnp.arange(entries.shape[position]) // (entries.shape[position] // shards_of)).reshape((-1,) + (1,) * (entries.ndim - 1 - position))

    near = jax.random.permutation(rng, shards_of)[block_of(target)]
    second = (block_of(target) + shards_of // 2) % shards_of
    return jnp.where((block_of(source) == near) | (block_of(source) == second), factor * entries, entries)


def shard_levels(own_key, extent, shards, least, top_value):
    def one(position, shards_of):
        steps = jax.random.uniform(jax.random.fold_in(jax.random.fold_in(own_key, 6), position), (shards_of,), jnp.float32, least / len(shards), top_value / len(shards))
        return jnp.repeat(jnp.exp(steps), extent[position] // shards_of).reshape((-1,) + (1,) * (len(extent) - position - 1))

    loudness = one(*shards[0])
    for cut in shards[1:]:
        loudness = loudness * one(*cut)
    return loudness


def noise(rng, dims, deviation, reach, shards=(), kind=jnp.bfloat16):
    array = jax.random.normal(rng, dims, jnp.float32) * deviation
    if len(shards) > 0:
        array = shard_levels(rng, dims, shards, -0.22, 0.18) * array
    return jnp.clip(array, min=-reach, max=reach).astype(kind)


def gaussian_with(stream_key, shape, scale, bound, cuts, heavy, kind=jnp.bfloat16):
    entries = scale * jax.random.normal(stream_key, shape, jnp.float32)
    if cuts:
        entries = entries * shard_levels(stream_key, shape, cuts, -0.22, 0.18)
    return jnp.clip(strengthened(entries, jax.random.fold_in(stream_key, 3), *heavy), -bound, bound).astype(kind)


def setup_inputs(seed: int = 0) -> dict:
    seeds = jax.random.split(jax.random.key(seed), 7)
    value_grad = gaussian_with(seeds[0], (2, TOKENS, F), 1.0, 6.0, ((0, 2), (1, 4), (2, 4)), (1, 2, 4, 2.0))
    stream = draw_stream(jax.random.fold_in(seeds[6], 71), 0)
    weights = noise(seeds[2], (2, F, D), D ** -0.5, 0.109375, ((0, 2), (1, 4)))
    gain = jnp.clip(1.0 + 0.15 * jax.random.normal(seeds[3], (2, D), jnp.float32), 0.25, 1.75)
    top_grad = noise(seeds[4], (TOKENS, D), 1.0, 6.0, ((0, 4),))
    counts = draw_counts(jax.random.fold_in(seeds[6], 71), 0)
    return {"value_grad": value_grad, "stream": stream, "weights": weights, "gain": gain, "top_grad": top_grad, "counts": counts}


def normalize(stream_rows):
    values = stream_rows.astype(jnp.float32)
    average = lax.optimization_barrier(jnp.mean(values, axis=-1, keepdims=True))
    centred = values - average
    variance = lax.optimization_barrier(jnp.mean(centred * centred, axis=-1, keepdims=True))
    inv_scale = lax.rsqrt(variance + 1e-06)
    return (centred * inv_scale, inv_scale)

def reference(value_grad, stream, weights, gain, top_grad, counts):
    per_replica = MICRO * TOK_MB
    token_index = jnp.arange(TOKENS, dtype=jnp.int32)
    replica = token_index // per_replica
    micro_index = token_index % per_replica // TOK_MB
    live_mask = (micro_index < counts[replica]).astype(jnp.bfloat16)
    block_rows = F // GROUPS
    weight_grads = []
    branch_terms = []
    for section_index in range(2):
        whitened, inv_scale = normalize(stream[section_index])
        gain_row = gain[section_index].astype(jnp.float32)
        normed = (whitened * gain_row).astype(jnp.bfloat16)
        masked = value_grad[section_index] * live_mask[:, None]
        weight_grads.append(jnp.dot(masked.T, normed, preferred_element_type=jnp.float32).astype(jnp.bfloat16))
        norm_grad = jnp.zeros((TOKENS, D), jnp.float32)
        for block_index in range(GROUPS):
            low = block_index * block_rows
            partial_value = jnp.dot(value_grad[section_index][:, low:low + block_rows], weights[section_index][low:low + block_rows], preferred_element_type=jnp.float32).astype(jnp.bfloat16)
            norm_grad = norm_grad + lax.optimization_barrier(partial_value).astype(jnp.float32)
        scaled_grad = norm_grad * gain_row
        first_mean = lax.optimization_barrier(jnp.mean(scaled_grad, axis=-1, keepdims=True))
        second_mean = lax.optimization_barrier(jnp.mean(scaled_grad * whitened, axis=-1, keepdims=True))
        branch_terms.append(inv_scale * (scaled_grad - first_mean - whitened * second_mean))
    above_grad = (top_grad.astype(jnp.float32) + branch_terms[1]).astype(jnp.bfloat16)
    lower_grad = (above_grad.astype(jnp.float32) + branch_terms[0]).astype(jnp.bfloat16)
    return (jnp.stack(weight_grads), jnp.stack([lower_grad, above_grad]))
```

```python
import functools

import jax
import jax.numpy as jnp
from jax import lax
from jax.experimental import pallas as pl
from jax.experimental.pallas import tpu as pltpu
from jax.sharding import PartitionSpec as P

TOK_MB = 256
LANES = 128
ROWS = 128
LN_ROWS = 64
EPS = 1e-06
F32 = jnp.float32
BF16 = jnp.bfloat16
MESH = pl.DeviceIdType.MESH


def kernel(
    dims,
    vg_hbm,
    st_hbm,
    w_hbm,
    gain_ref,
    top_hbm,
    counts_ref,
    wg_ref,
    res_ref,
    vg_v,
    st_v,
    w_v,
    top_v,
    mean_v,
    inv_v,
    nrm,
    nrm_in,
    vgt,
    vgt_in,
    ssend,
    srecv,
    rt,
    psend,
    precv,
    acc,
    sums,
    sums_in,
    above_in,
    branch_v,
    load_sem,
    n_send,
    n_recv,
    fwd_send,
    vgt_send,
    vgt_recv,
    s_send,
    s_recv,
    rt_send,
    wg_recv,
    p_send,
    p_recv,
    sum_send,
    sum_recv,
    above_send,
    above_recv,
):
    tokens, width, feats, quarter, out_rows = dims
    blocks = width // LANES
    per_quarter = quarter // LANES
    chunks = tokens // ROWS
    sec = lax.axis_index("section")
    m = lax.axis_index("mp")
    z = lax.axis_index("dp")
    inner = lax.rem(z, 3) != 0
    outer = lax.rem(z, 3) == 0
    mate = z + 1 - 2 * lax.rem(z, 2)
    cross = 3 - z
    keep_half = z // 2
    give_half = 1 - z // 2
    own_slot = lax.rem(z, 2)
    mate_slot = 1 - own_slot

    def peer(kk):
        row = lax.rem(m // 2 + kk // 2, 2)
        col = lax.rem(lax.rem(m, 2) + lax.rem(kk, 2), 2)
        return 2 * row + col

    def column(kk, idx):
        return peer(kk) * per_quarter + idx

    def lanes(start, size=LANES):
        return pl.ds(pl.multiple_of(start, LANES), size)

    def row_chunk(i):
        return pl.ds(pl.multiple_of(i * ROWS, ROWS), ROWS)

    def remote(src, dst, send, recv, where):
        return pltpu.make_async_remote_copy(
            src_ref=src,
            dst_ref=dst,
            send_sem=send,
            recv_sem=recv,
            device_id=where,
            device_id_type=MESH,
        )

    load_vg = pltpu.make_async_copy(vg_hbm.at[0], vg_v, load_sem.at[0])
    load_vg.start()
    load_st = pltpu.make_async_copy(st_hbm.at[0], st_v, load_sem.at[1])
    load_st.start()

    def load_w(kk):
        return pltpu.make_async_copy(
            w_hbm.at[0, :, lanes(peer(kk) * quarter, quarter)],
            w_v.at[kk],
            load_sem.at[2 + kk],
        )

    for kk in (3, 2, 1, 0):
        load_w(kk).start()
    load_top = pltpu.make_async_copy(
        top_hbm.at[:, lanes(m * quarter, quarter)], top_v, load_sem.at[6]
    )
    load_top.start()

    barrier = pltpu.get_barrier_semaphore()

    def greet(where):
        pl.semaphore_signal(barrier, inc=1, device_id=where, device_id_type=MESH)

    for kk in (1, 2, 3):
        greet({"mp": peer(kk)})
    greet({"dp": mate})
    greet({"section": 1 - sec})

    @pl.when(inner)
    def _():
        greet({"dp": cross})
        pl.semaphore_wait(barrier, 6)

    @pl.when(outer)
    def _():
        pl.semaphore_wait(barrier, 5)

    load_vg.wait()
    half = feats // 2
    for h in range(2):
        vgt[h] = vg_v[:, h * half : (h + 1) * half].T

    def copy_vgt(h):
        return remote(
            vgt.at[h], vgt_in.at[h], vgt_send.at[h], vgt_recv.at[h], {"dp": mate}
        )

    @pl.when(outer)
    def _():
        copy_vgt(give_half).start()

    load_st.wait()
    live_count = counts_ref[0]

    def norm_chunk(i, carry):
        first = pl.multiple_of(i * LN_ROWS, LN_ROWS)
        rows = pl.ds(first, LN_ROWS)
        total = jnp.zeros((LN_ROWS, LANES), F32)
        for t in range(blocks):
            total = total + st_v[rows, t * LANES : (t + 1) * LANES].astype(F32)
        mean = jnp.sum(total, axis=-1, keepdims=True) * (1.0 / width)
        mean = jnp.broadcast_to(mean, (LN_ROWS, LANES))
        total = jnp.zeros((LN_ROWS, LANES), F32)
        for t in range(blocks):
            centred = st_v[rows, t * LANES : (t + 1) * LANES].astype(F32) - mean
            total = total + centred * centred
        var = jnp.sum(total, axis=-1, keepdims=True) * (1.0 / width)
        inv = jnp.broadcast_to(lax.rsqrt(var + EPS), (LN_ROWS, LANES))
        mean_v[rows] = mean
        inv_v[rows] = inv
        live = (first // TOK_MB < live_count).astype(F32)
        scale = inv * live
        for t in range(blocks):
            cols = slice(t * LANES, (t + 1) * LANES)
            white = (st_v[rows, cols].astype(F32) - mean) * scale
            nrm[t, rows] = (white * gain_ref[:, cols]).astype(BF16)
        return carry

    lax.fori_loop(0, tokens // LN_ROWS, norm_chunk, 0)

    def copy_normed(kk, idx):
        c = column(kk, idx)
        return remote(
            nrm.at[c], nrm_in.at[c], n_send.at[c], n_recv.at[c], {"dp": mate}
        )

    @pl.when(outer)
    def _():
        def send_pair(idx, carry):
            copy_normed(0, idx).start()
            copy_normed(3, idx).start()
            return carry

        lax.fori_loop(0, per_quarter, send_pair, 0)
        copy_vgt(keep_half).start()

    def copy_part(kk, chunk):
        rows = row_chunk(chunk)
        return remote(
            psend.at[kk, rows],
            precv.at[kk, rows],
            p_send.at[kk, chunk],
            p_recv.at[kk, chunk],
            {"mp": peer(kk)},
        )

    acc[...] = jnp.zeros_like(acc)

    def part_step(s, carry):
        kk = 3 - s // chunks
        chunk = lax.rem(s, chunks)
        rows = row_chunk(chunk)
        q = peer(kk)

        @pl.when(chunk == 0)
        def _():
            load_w(kk).wait()

        part = jnp.dot(vg_v[rows], w_v[kk], preferred_element_type=F32).astype(BF16)
        psend[kk, rows] = part
        first = jnp.zeros((ROWS, LANES), F32)
        second = jnp.zeros((ROWS, LANES), F32)
        mean = mean_v[rows]
        inv = inv_v[rows]
        for j in range(per_quarter):
            cols = lanes(q * quarter + j * LANES)
            local = part[:, j * LANES : (j + 1) * LANES].astype(F32) * gain_ref[:, cols]
            white = (st_v[rows, cols].astype(F32) - mean) * inv
            first = first + local
            second = second + local * white
        acc[0, rows] += first
        acc[1, rows] += second

        @pl.when(kk > 0)
        def _():
            copy_part(kk, chunk).start()

        return carry

    lax.fori_loop(0, 4 * chunks, part_step, 0)

    lane = lax.broadcasted_iota(jnp.int32, (tokens, LANES), 1)
    sum0 = jnp.sum(acc[0], axis=-1, keepdims=True)
    sum1 = jnp.sum(acc[1], axis=-1, keepdims=True)
    packed = jnp.where(lane == 0, sum0, jnp.where(lane == 1, sum1, 0.0))
    sums[...] = packed.T[:8]

    def copy_sums(kk):
        return remote(
            sums, sums_in.at[kk], sum_send.at[kk], sum_recv.at[kk], {"mp": peer(kk)}
        )

    for kk in (3, 2, 1):
        copy_sums(kk).start()

    def copy_above(chunk):
        rows = row_chunk(chunk)
        return remote(
            res_ref.at[rows],
            above_in.at[rows],
            above_send.at[chunk],
            above_recv.at[chunk],
            {"section": 1 - sec},
        )

    def residual():
        load_top.wait()
        for kk in (1, 2, 3):
            copy_sums(kk).wait_recv()
        total = (sums[...] + sums_in[1]) + (sums_in[2] + sums_in[3])
        total = jnp.concatenate([total] * (LANES // 8), axis=0) * (1.0 / width)
        total = total.T
        acc[0] = jnp.broadcast_to(total[:, 0:1], (tokens, LANES))
        acc[1] = jnp.broadcast_to(total[:, 1:2], (tokens, LANES))

        def rows_step(chunk, carry):
            rows = row_chunk(chunk)
            for kk in (1, 2, 3):
                copy_part(kk, chunk).wait_recv()
            mean = mean_v[rows]
            inv = inv_v[rows]
            for j in range(per_quarter):
                here = slice(j * LANES, (j + 1) * LANES)
                cols = lanes(m * quarter + j * LANES)
                grad = psend[0, rows, here].astype(F32)
                for kk in (1, 2, 3):
                    grad = grad + precv[kk, rows, here].astype(F32)
                scaled = grad * gain_ref[:, cols]
                white = (st_v[rows, cols].astype(F32) - mean) * inv
                branch = inv * (scaled - acc[0, rows] - white * acc[1, rows])
                branch_v[rows, here] = branch
                res_ref[rows, here] = (top_v[rows, here].astype(F32) + branch).astype(
                    BF16
                )

            @pl.when(sec == 1)
            def _():
                copy_above(chunk).start()

            return carry

        lax.fori_loop(0, chunks, rows_step, 0)

        @pl.when(sec == 0)
        def _():
            def lower(chunk, carry):
                rows = row_chunk(chunk)
                copy_above(chunk).wait_recv()
                res_ref[rows] = (above_in[rows].astype(F32) + branch_v[rows]).astype(
                    BF16
                )
                return carry

            lax.fori_loop(0, chunks, lower, 0)

    def copy_wg(c):
        return remote(
            rt.at[c, mate_slot],
            wg_ref.at[:, lanes(c * LANES)],
            rt_send.at[c],
            wg_recv.at[c],
            {"dp": mate},
        )

    @pl.when(outer)
    def _():
        residual()

        def finish(c, carry):
            copy_wg(c).wait_recv()
            return carry

        lax.fori_loop(0, blocks, finish, 0)
        for h in range(2):
            copy_vgt(h).wait_send()

        def sent(idx, carry):
            copy_normed(0, idx).wait_send()
            copy_normed(3, idx).wait_send()
            return carry

        lax.fori_loop(0, per_quarter, sent, 0)

    @pl.when(inner)
    def _():
        def copy_forward(kk, idx):
            c = column(0, idx)
            return remote(
                nrm_in.at[c],
                nrm_in.at[c],
                fwd_send.at[kk - 1, idx],
                n_recv.at[c],
                {"mp": peer(kk)},
            )

        def copy_cross(c):
            return remote(
                ssend.at[c], srecv.at[c], s_send.at[c], s_recv.at[c], {"dp": cross}
            )

        def wait_normed(c):
            remote(
                nrm.at[c], nrm_in.at[c], n_send.at[c], n_recv.at[c], {"dp": mate}
            ).wait_recv()

        def forward(idx):
            wait_normed(column(0, idx))
            copy_forward(1, idx).start()
            copy_forward(2, idx).start()

        def column_at(i):
            return column(lax.rem(3 * lax.rem(i, 4), 4), i // 4)

        def product(h, c):
            return jnp.dot(vgt[h], nrm[c], preferred_element_type=F32) + jnp.dot(
                vgt_in[h], nrm_in[c], preferred_element_type=F32
            )

        def give(i):
            c = column_at(i)

            @pl.when(lax.rem(i, 4) != 0)
            def _():
                wait_normed(c)

            ssend[c] = product(give_half, c).astype(BF16)
            copy_cross(c).start()

            @pl.when(jnp.logical_and(lax.rem(i, 4) == 3, i < blocks - 4))
            def _():
                forward(i // 4 + 1)

        def keep(i):
            c = column_at(i)
            copy_cross(c).wait_recv()
            total = product(keep_half, c) + srecv[c].astype(F32)
            total = total.astype(BF16)
            rt[c, 0] = total[:out_rows]
            rt[c, 1] = total[out_rows:]
            copy_wg(c).start()
            wg_ref[:, lanes(c * LANES)] = rt[c, own_slot]

        copy_vgt(give_half).wait_recv()
        forward(0)

        def first_round(i, carry):
            give(i)
            return carry

        lax.fori_loop(0, 4, first_round, 0)
        copy_give_wait = copy_vgt(keep_half)
        give(4)
        give(5)
        give(6)
        give(7)
        copy_give_wait.wait_recv()

        def both(i, carry):
            give(i)
            keep(i - 8)
            return carry

        lax.fori_loop(8, blocks, both, 0)
        residual()

        def last(i, carry):
            keep(i)
            return carry

        lax.fori_loop(blocks - 8, blocks, last, 0)

        def sent(c, carry):
            copy_cross(c).wait_send()
            copy_wg(c).wait_send()
            return carry

        lax.fori_loop(0, blocks, sent, 0)

        def forwarded(idx, carry):
            copy_forward(1, idx).wait_send()
            copy_forward(2, idx).wait_send()
            return carry

        lax.fori_loop(0, per_quarter, forwarded, 0)

    for kk in (1, 2, 3):
        copy_sums(kk).wait_send()

        def part_sent(chunk, carry):
            copy_part(kk, chunk).wait_send()
            return carry

        lax.fori_loop(0, chunks, part_sent, 0)

    @pl.when(sec == 1)
    def _():
        def above_sent(chunk, carry):
            copy_above(chunk).wait_send()
            return carry

        lax.fori_loop(0, chunks, above_sent, 0)


def fused(value_grad, stream, weights, gain, top_grad, counts):
    tokens, width = stream.shape[1:]
    feats = value_grad.shape[2]
    quarter = width // lax.axis_size("mp")
    out_rows = feats // lax.axis_size("dp")
    blocks = width // LANES
    per_quarter = quarter // LANES
    chunks = tokens // ROWS
    dma = pltpu.SemaphoreType.DMA
    vmem = pltpu.VMEM
    anywhere = pl.BlockSpec(memory_space=pl.ANY)
    in_vmem = pl.BlockSpec(memory_space=pltpu.VMEM)
    weight_grad, residual_grad = pl.pallas_call(
        functools.partial(kernel, (tokens, width, feats, quarter, out_rows)),
        out_shape=(
            jax.ShapeDtypeStruct((out_rows, width), BF16),
            jax.ShapeDtypeStruct((tokens, quarter), BF16),
        ),
        in_specs=[
            anywhere,
            anywhere,
            anywhere,
            in_vmem,
            anywhere,
            pl.BlockSpec(memory_space=pltpu.SMEM),
        ],
        out_specs=(in_vmem, in_vmem),
        scratch_shapes=[
            vmem((tokens, feats), BF16),
            vmem((tokens, width), BF16),
            vmem((4, feats, quarter), BF16),
            vmem((tokens, quarter), BF16),
            vmem((tokens, LANES), F32),
            vmem((tokens, LANES), F32),
            vmem((blocks, tokens, LANES), BF16),
            vmem((blocks, tokens, LANES), BF16),
            vmem((2, feats // 2, tokens), BF16),
            vmem((2, feats // 2, tokens), BF16),
            vmem((blocks, 2 * out_rows, LANES), BF16),
            vmem((blocks, 2 * out_rows, LANES), BF16),
            vmem((blocks, 2, out_rows, LANES), BF16),
            vmem((4, tokens, quarter), BF16),
            vmem((4, tokens, quarter), BF16),
            vmem((2, tokens, LANES), F32),
            vmem((8, tokens), F32),
            vmem((4, 8, tokens), F32),
            vmem((tokens, quarter), BF16),
            vmem((tokens, quarter), F32),
            dma((7,)),
            dma((blocks,)),
            dma((blocks,)),
            dma((2, per_quarter)),
            dma((2,)),
            dma((2,)),
            dma((blocks,)),
            dma((blocks,)),
            dma((blocks,)),
            dma((blocks,)),
            dma((4, chunks)),
            dma((4, chunks)),
            dma((4,)),
            dma((4,)),
            dma((chunks,)),
            dma((chunks,)),
        ],
        compiler_params=pltpu.CompilerParams(
            collective_id=0, has_side_effects=True, vmem_limit_bytes=52 * 2**20
        ),
    )(value_grad, stream, weights, gain, top_grad, counts)
    return weight_grad[None], residual_grad[None]


def normalize(stream_rows):
    values = stream_rows.astype(F32)
    average = jnp.mean(values, axis=-1, keepdims=True)
    centred = values - average
    variance = jnp.mean(centred * centred, axis=-1, keepdims=True)
    inv_scale = lax.rsqrt(variance + EPS)
    return (centred * inv_scale, inv_scale)


def collectives(value_grad, stream, weights, gain, top_grad, counts):
    section_index = lax.axis_index("section")
    model_index = lax.axis_index("mp")
    row_total = stream.shape[1]
    whitened, inv_scale = normalize(stream[0])
    gain_row = gain[0]
    width = whitened.shape[1]
    share = width // lax.axis_size("mp")
    first_col = model_index * share
    cols = lambda a: lax.dynamic_slice_in_dim(a, first_col, share, 1)
    partial = jnp.dot(value_grad[0], weights[0], preferred_element_type=F32)
    partial = partial.astype(BF16)
    local = partial.astype(F32) * gain_row
    sums = jnp.stack([jnp.sum(local, -1), jnp.sum(local * whitened, -1)])
    norm_grad = lax.psum_scatter(partial, "mp", scatter_dimension=1, tiled=True)
    sums = lax.psum(sums, "mp") * (1.0 / width)
    normed = (whitened * gain_row).astype(BF16)
    micro_index = jnp.arange(row_total, dtype=jnp.int32) // TOK_MB
    live_mask = (micro_index < counts[0]).astype(BF16)
    masked = value_grad[0] * live_mask[:, None]
    product = lax.dot_general(
        masked, normed, (((0,), (0,)), ((), ())), preferred_element_type=F32
    )
    weight_grad = lax.psum_scatter(
        product.astype(BF16), "dp", scatter_dimension=0, tiled=True
    )[None]
    scaled = norm_grad.astype(F32) * cols(gain)
    branch = inv_scale * (scaled - sums[0][:, None] - cols(whitened) * sums[1][:, None])
    above = (cols(top_grad).astype(F32) + branch).astype(BF16)
    below = lax.ppermute(above, "section", [(1, 0)])
    lower = (below.astype(F32) + branch).astype(BF16)
    result = jnp.where(section_index == 0, lower, above)
    return (weight_grad, result[None])


def solution(mesh):
    in_specs = (
        P("section", "dp", "mp"),
        P("section", "dp", None),
        P("section", "mp", None),
        P("section", None),
        P("dp", None),
        P("dp"),
    )
    out_specs = (P("section", ("mp", "dp"), None), P("section", "dp", "mp"))
    grid = (mesh.shape["section"], mesh.shape["mp"], mesh.shape["dp"])
    step = fused if grid == (2, 4, 4) else collectives
    return jax.shard_map(step, mesh=mesh, in_specs=in_specs, out_specs=out_specs, check_vma=False)
```

```python
import functools

import jax
import jax.numpy as jnp
from jax import lax
from jax.experimental import pallas as pl
from jax.experimental.pallas import tpu as pltpu
from jax.sharding import PartitionSpec as P

TOK_MB = 256
LANES = 128
ROWS = 128
LN_ROWS = 64
EPS = 1e-06
F32 = jnp.float32
BF16 = jnp.bfloat16
MESH = pl.DeviceIdType.MESH


def kernel(
    dims,
    vg_hbm,
    st_hbm,
    w_hbm,
    gain_hbm,
    top_hbm,
    counts_ref,
    wg_ref,
    res_ref,
    vg_v,
    st_v,
    w_v,
    top_v,
    gain_ref,
    mean_v,
    inv_v,
    nrm,
    nrm_in,
    vgt,
    vgt_in,
    ssend,
    srecv,
    rt,
    psend,
    precv,
    acc,
    sums,
    sums_in,
    above_in,
    branch_v,
    load_sem,
    n_send,
    n_recv,
    fwd_send,
    vgt_send,
    vgt_recv,
    s_send,
    s_recv,
    rt_send,
    wg_recv,
    p_send,
    p_recv,
    sum_send,
    sum_recv,
    above_send,
    above_recv,
):
    tokens, width, feats, quarter, out_rows = dims
    blocks = width // LANES
    per_quarter = quarter // LANES
    chunks = tokens // ROWS
    sec = lax.axis_index("section")
    m = lax.axis_index("mp")
    z = lax.axis_index("dp")
    inner = lax.rem(z, 3) != 0
    outer = lax.rem(z, 3) == 0
    mate = z + 1 - 2 * lax.rem(z, 2)
    cross = 3 - z
    keep_half = z // 2
    give_half = 1 - z // 2
    own_slot = lax.rem(z, 2)
    mate_slot = 1 - own_slot

    def peer(kk):
        row = lax.rem(m // 2 + kk // 2, 2)
        col = lax.rem(lax.rem(m, 2) + lax.rem(kk, 2), 2)
        return 2 * row + col

    def column(kk, idx):
        return peer(kk) * per_quarter + idx

    def lanes(start, size=LANES):
        return pl.ds(pl.multiple_of(start, LANES), size)

    def row_chunk(i):
        return pl.ds(pl.multiple_of(i * ROWS, ROWS), ROWS)

    def remote(src, dst, send, recv, where):
        return pltpu.make_async_remote_copy(
            src_ref=src,
            dst_ref=dst,
            send_sem=send,
            recv_sem=recv,
            device_id=where,
            device_id_type=MESH,
        )

    load_vg = pltpu.make_async_copy(vg_hbm.at[0], vg_v, load_sem.at[0])
    load_vg.start()
    load_st = pltpu.make_async_copy(st_hbm.at[0], st_v, load_sem.at[1])
    load_st.start()
    load_gain = pltpu.make_async_copy(gain_hbm, gain_ref, load_sem.at[7])
    load_gain.start()

    def load_w(kk):
        return pltpu.make_async_copy(
            w_hbm.at[0, :, lanes(peer(kk) * quarter, quarter)],
            w_v.at[kk],
            load_sem.at[2 + kk],
        )

    for kk in (3, 2, 1, 0):
        load_w(kk).start()
    load_top = pltpu.make_async_copy(
        top_hbm.at[:, lanes(m * quarter, quarter)], top_v, load_sem.at[6]
    )
    load_top.start()

    barrier = pltpu.get_barrier_semaphore()

    def greet(where):
        pl.semaphore_signal(barrier, inc=1, device_id=where, device_id_type=MESH)

    for kk in (1, 2, 3):
        greet({"mp": peer(kk)})
    greet({"dp": mate})
    greet({"section": 1 - sec})

    @pl.when(inner)
    def _():
        greet({"dp": cross})
        pl.semaphore_wait(barrier, 6)

    @pl.when(outer)
    def _():
        pl.semaphore_wait(barrier, 5)

    load_vg.wait()
    half = feats // 2
    for h in range(2):
        vgt[h] = vg_v[:, h * half : (h + 1) * half].T

    def copy_vgt(h):
        return remote(
            vgt.at[h], vgt_in.at[h], vgt_send.at[h], vgt_recv.at[h], {"dp": mate}
        )

    early = jnp.logical_and(outer, sec == 0)
    late = jnp.logical_and(outer, sec == 1)

    @pl.when(early)
    def _():
        copy_vgt(give_half).start()

    load_gain.wait()
    load_st.wait()
    live_count = counts_ref[0]

    def norm_chunk(i, carry):
        first = pl.multiple_of(i * LN_ROWS, LN_ROWS)
        rows = pl.ds(first, LN_ROWS)
        total = jnp.zeros((LN_ROWS, LANES), F32)
        for t in range(blocks):
            total = total + st_v[rows, t * LANES : (t + 1) * LANES].astype(F32)
        mean = jnp.sum(total, axis=-1, keepdims=True) * (1.0 / width)
        mean = jnp.broadcast_to(mean, (LN_ROWS, LANES))
        total = jnp.zeros((LN_ROWS, LANES), F32)
        for t in range(blocks):
            centred = st_v[rows, t * LANES : (t + 1) * LANES].astype(F32) - mean
            total = total + centred * centred
        var = jnp.sum(total, axis=-1, keepdims=True) * (1.0 / width)
        inv = jnp.broadcast_to(lax.rsqrt(var + EPS), (LN_ROWS, LANES))
        mean_v[rows] = mean
        inv_v[rows] = inv
        live = (first // TOK_MB < live_count).astype(F32)
        scale = inv * live
        for t in range(blocks):
            cols = slice(t * LANES, (t + 1) * LANES)
            white = (st_v[rows, cols].astype(F32) - mean) * scale
            nrm[t, rows] = (white * gain_ref[:, cols]).astype(BF16)
        return carry

    lax.fori_loop(0, tokens // LN_ROWS, norm_chunk, 0)

    def copy_normed(kk, idx):
        c = column(kk, idx)
        return remote(
            nrm.at[c], nrm_in.at[c], n_send.at[c], n_recv.at[c], {"dp": mate}
        )

    split = per_quarter - 2

    def send_normed():
        def send_pair(idx, carry):
            copy_normed(0, idx).start()
            copy_normed(3, idx).start()
            return carry

        lax.fori_loop(0, split, send_pair, 0)
        copy_vgt(keep_half).start()
        lax.fori_loop(split, per_quarter, send_pair, 0)

    @pl.when(early)
    def _():
        send_normed()

    upper = chunks // 2
    hold = jnp.logical_and(inner, sec == 0)

    def copy_part(kk, chunk):
        rows = row_chunk(chunk)
        first_hop = 1 + chunk // upper
        hop = jnp.where(kk == 3, first_hop, kk)
        return remote(
            psend.at[kk, rows],
            precv.at[kk, rows],
            p_send.at[kk, chunk],
            p_recv.at[kk, chunk],
            {"mp": peer(hop)},
        )

    def pass_on(chunk):
        rows = row_chunk(chunk)
        kk = 2 - chunk // upper
        copy_part(3, chunk).wait_recv()
        psend[kk, rows] = (psend[kk, rows].astype(F32) + precv[3, rows].astype(F32)).astype(BF16)
        copy_part(kk, chunk).start()

    def pass_all():
        def one(chunk, carry):
            pass_on(chunk)
            return carry

        lax.fori_loop(0, chunks, one, 0)

    acc[...] = jnp.zeros_like(acc)

    def part_step(s, carry):
        kk = 3 - s // chunks
        chunk = lax.rem(s, chunks)
        rows = row_chunk(chunk)
        q = peer(kk)

        @pl.when(chunk == 0)
        def _():
            load_w(kk).wait()

        part = jnp.dot(vg_v[rows], w_v[kk], preferred_element_type=F32).astype(BF16)
        psend[kk, rows] = part
        first = jnp.zeros((ROWS, LANES), F32)
        second = jnp.zeros((ROWS, LANES), F32)
        mean = mean_v[rows]
        inv = inv_v[rows]
        for j in range(per_quarter):
            cols = lanes(q * quarter + j * LANES)
            local = part[:, j * LANES : (j + 1) * LANES].astype(F32) * gain_ref[:, cols]
            white = (st_v[rows, cols].astype(F32) - mean) * inv
            first = first + local
            second = second + local * white
        acc[0, rows] += first
        acc[1, rows] += second

        direct = jnp.logical_or(kk == 3, kk == 1 + chunk // upper)

        @pl.when(jnp.logical_and(direct, jnp.logical_or(outer, sec == 1)))
        def _():
            copy_part(kk, chunk).start()

        return carry

    lax.fori_loop(0, 4 * chunks, part_step, 0)

    @pl.when(late)
    def _():
        copy_vgt(give_half).start()
        send_normed()

    lane = lax.broadcasted_iota(jnp.int32, (tokens, LANES), 1)
    sum0 = jnp.sum(acc[0], axis=-1, keepdims=True)
    sum1 = jnp.sum(acc[1], axis=-1, keepdims=True)
    packed = jnp.where(lane == 0, sum0, jnp.where(lane == 1, sum1, 0.0))
    sums[...] = packed.T[:8]

    def copy_sums(kk):
        return remote(
            sums, sums_in.at[kk], sum_send.at[kk], sum_recv.at[kk], {"mp": peer(kk)}
        )

    for kk in (3, 2, 1):
        copy_sums(kk).start()

    @pl.when(jnp.logical_or(outer, sec == 1))
    def _():
        pass_all()

    def copy_above(chunk):
        rows = row_chunk(chunk)
        return remote(
            res_ref.at[rows],
            above_in.at[rows],
            above_send.at[chunk],
            above_recv.at[chunk],
            {"section": 1 - sec},
        )

    def residual():
        load_top.wait()
        for kk in (1, 2, 3):
            copy_sums(kk).wait_recv()
        total = (sums[...] + sums_in[1]) + (sums_in[2] + sums_in[3])
        total = jnp.concatenate([total] * (LANES // 8), axis=0) * (1.0 / width)
        total = total.T
        acc[0] = jnp.broadcast_to(total[:, 0:1], (tokens, LANES))
        acc[1] = jnp.broadcast_to(total[:, 1:2], (tokens, LANES))

        def rows_step(chunk, carry):
            rows = row_chunk(chunk)
            for kk in (1, 2):
                copy_part(kk, chunk).wait_recv()
            mean = mean_v[rows]
            inv = inv_v[rows]
            for j in range(per_quarter):
                here = slice(j * LANES, (j + 1) * LANES)
                cols = lanes(m * quarter + j * LANES)
                grad = psend[0, rows, here].astype(F32)
                for kk in (1, 2):
                    grad = grad + precv[kk, rows, here].astype(F32)
                scaled = grad * gain_ref[:, cols]
                white = (st_v[rows, cols].astype(F32) - mean) * inv
                branch = inv * (scaled - acc[0, rows] - white * acc[1, rows])
                branch_v[rows, here] = branch
                res_ref[rows, here] = (top_v[rows, here].astype(F32) + branch).astype(
                    BF16
                )

            @pl.when(sec == 1)
            def _():
                copy_above(chunk).start()

            return carry

        lax.fori_loop(0, chunks, rows_step, 0)

        @pl.when(sec == 0)
        def _():
            def lower(chunk, carry):
                rows = row_chunk(chunk)
                copy_above(chunk).wait_recv()
                res_ref[rows] = (above_in[rows].astype(F32) + branch_v[rows]).astype(
                    BF16
                )
                return carry

            lax.fori_loop(0, chunks, lower, 0)

    def copy_wg(c):
        return remote(
            rt.at[c, mate_slot],
            wg_ref.at[:, lanes(c * LANES)],
            rt_send.at[c],
            wg_recv.at[c],
            {"dp": mate},
        )

    @pl.when(outer)
    def _():
        residual()

        def finish(c, carry):
            copy_wg(c).wait_recv()
            return carry

        lax.fori_loop(0, blocks, finish, 0)
        for h in range(2):
            copy_vgt(h).wait_send()

        def sent(idx, carry):
            copy_normed(0, idx).wait_send()
            copy_normed(3, idx).wait_send()
            return carry

        lax.fori_loop(0, per_quarter, sent, 0)

    @pl.when(inner)
    def _():
        def copy_forward(kk, idx):
            c = column(0, idx)
            return remote(
                nrm_in.at[c],
                nrm_in.at[c],
                fwd_send.at[kk - 1, idx],
                n_recv.at[c],
                {"mp": peer(kk)},
            )

        def copy_cross(c):
            return remote(
                ssend.at[c], srecv.at[c], s_send.at[c], s_recv.at[c], {"dp": cross}
            )

        def wait_normed(c):
            remote(
                nrm.at[c], nrm_in.at[c], n_send.at[c], n_recv.at[c], {"dp": mate}
            ).wait_recv()

        def forward(idx):
            wait_normed(column(0, idx))
            copy_forward(1, idx).start()
            copy_forward(2, idx).start()

        def column_at(i):
            return column(lax.rem(3 * lax.rem(i, 4), 4), i // 4)

        def product(h, c):
            return jnp.dot(vgt[h], nrm[c], preferred_element_type=F32) + jnp.dot(
                vgt_in[h], nrm_in[c], preferred_element_type=F32
            )

        def give(i):
            c = column_at(i)

            @pl.when(lax.rem(i, 4) != 0)
            def _():
                wait_normed(c)

            ssend[c] = product(give_half, c).astype(BF16)
            copy_cross(c).start()

            @pl.when(jnp.logical_and(lax.rem(i, 4) == 3, i < blocks - 4))
            def _():
                forward(i // 4 + 1)

            @pl.when(jnp.logical_and(hold, i == 3))
            def _():
                for chunk in range(0, chunks, 2):
                    copy_part(3, chunk).start()

            @pl.when(jnp.logical_and(hold, i == 7))
            def _():
                for chunk in range(1, chunks, 2):
                    copy_part(3, chunk).start()

            @pl.when(jnp.logical_and(hold, i == 11))
            def _():
                for chunk in range(chunks):
                    copy_part(1 + chunk // upper, chunk).start()

            @pl.when(jnp.logical_and(hold, i == 14))
            def _():
                pass_all()

        def keep(i):
            c = column_at(i)
            copy_cross(c).wait_recv()
            total = product(keep_half, c) + srecv[c].astype(F32)
            total = total.astype(BF16)
            rt[c, 0] = total[:out_rows]
            rt[c, 1] = total[out_rows:]
            copy_wg(c).start()
            wg_ref[:, lanes(c * LANES)] = rt[c, own_slot]

        copy_vgt(give_half).wait_recv()
        forward(0)

        head = 4 * split

        def first(i, carry):
            give(i)
            return carry

        lax.fori_loop(0, head, first, 0)
        copy_vgt(keep_half).wait_recv()

        def both(i, carry):
            give(i)
            keep(2 * (i - head))
            keep(2 * (i - head) + 1)
            return carry

        lax.fori_loop(head, blocks, both, 0)
        residual()

        def last(i, carry):
            keep(i)
            return carry

        lax.fori_loop(2 * (blocks - head), blocks, last, 0)

        def sent(c, carry):
            copy_cross(c).wait_send()
            copy_wg(c).wait_send()
            return carry

        lax.fori_loop(0, blocks, sent, 0)

        def forwarded(idx, carry):
            copy_forward(1, idx).wait_send()
            copy_forward(2, idx).wait_send()
            return carry

        lax.fori_loop(0, per_quarter, forwarded, 0)

    for kk in (1, 2, 3):
        copy_sums(kk).wait_send()

        def part_sent(chunk, carry):
            copy_part(kk, chunk).wait_send()
            return carry

        lax.fori_loop(0, chunks, part_sent, 0)

    @pl.when(sec == 1)
    def _():
        def above_sent(chunk, carry):
            copy_above(chunk).wait_send()
            return carry

        lax.fori_loop(0, chunks, above_sent, 0)


def fused(value_grad, stream, weights, gain, top_grad, counts):
    tokens, width = stream.shape[1:]
    feats = value_grad.shape[2]
    quarter = width // lax.axis_size("mp")
    out_rows = feats // lax.axis_size("dp")
    blocks = width // LANES
    per_quarter = quarter // LANES
    chunks = tokens // ROWS
    dma = pltpu.SemaphoreType.DMA
    vmem = pltpu.VMEM
    in_hbm = pl.BlockSpec(memory_space=pltpu.HBM)
    in_vmem = pl.BlockSpec(memory_space=pltpu.VMEM)
    weight_grad, residual_grad = pl.pallas_call(
        functools.partial(kernel, (tokens, width, feats, quarter, out_rows)),
        out_shape=(
            jax.ShapeDtypeStruct((out_rows, width), BF16),
            jax.ShapeDtypeStruct((tokens, quarter), BF16),
        ),
        in_specs=[
            in_hbm,
            in_hbm,
            in_hbm,
            in_hbm,
            in_hbm,
            pl.BlockSpec(memory_space=pltpu.SMEM),
        ],
        out_specs=(in_vmem, in_vmem),
        scratch_shapes=[
            vmem((tokens, feats), BF16),
            vmem((tokens, width), BF16),
            vmem((4, feats, quarter), BF16),
            vmem((tokens, quarter), BF16),
            vmem((1, width), F32),
            vmem((tokens, LANES), F32),
            vmem((tokens, LANES), F32),
            vmem((blocks, tokens, LANES), BF16),
            vmem((blocks, tokens, LANES), BF16),
            vmem((2, feats // 2, tokens), BF16),
            vmem((2, feats // 2, tokens), BF16),
            vmem((blocks, 2 * out_rows, LANES), BF16),
            vmem((blocks, 2 * out_rows, LANES), BF16),
            vmem((blocks, 2, out_rows, LANES), BF16),
            vmem((4, tokens, quarter), BF16),
            vmem((4, tokens, quarter), BF16),
            vmem((2, tokens, LANES), F32),
            vmem((8, tokens), F32),
            vmem((4, 8, tokens), F32),
            vmem((tokens, quarter), BF16),
            vmem((tokens, quarter), F32),
            dma((8,)),
            dma((blocks,)),
            dma((blocks,)),
            dma((2, per_quarter)),
            dma((2,)),
            dma((2,)),
            dma((blocks,)),
            dma((blocks,)),
            dma((blocks,)),
            dma((blocks,)),
            dma((4, chunks)),
            dma((4, chunks)),
            dma((4,)),
            dma((4,)),
            dma((chunks,)),
            dma((chunks,)),
        ],
        compiler_params=pltpu.CompilerParams(
            collective_id=0, has_side_effects=True, vmem_limit_bytes=44 * 2**20
        ),
    )(value_grad, stream, weights, gain, top_grad, counts)
    return weight_grad[None], residual_grad[None]


def normalize(stream_rows):
    values = stream_rows.astype(F32)
    average = jnp.mean(values, axis=-1, keepdims=True)
    centred = values - average
    variance = jnp.mean(centred * centred, axis=-1, keepdims=True)
    inv_scale = lax.rsqrt(variance + EPS)
    return (centred * inv_scale, inv_scale)


def collectives(value_grad, stream, weights, gain, top_grad, counts):
    section_index = lax.axis_index("section")
    model_index = lax.axis_index("mp")
    row_total = stream.shape[1]
    whitened, inv_scale = normalize(stream[0])
    gain_row = gain[0]
    width = whitened.shape[1]
    share = width // lax.axis_size("mp")
    first_col = model_index * share
    cols = lambda a: lax.dynamic_slice_in_dim(a, first_col, share, 1)
    partial = jnp.dot(value_grad[0], weights[0], preferred_element_type=F32)
    partial = partial.astype(BF16)
    local = partial.astype(F32) * gain_row
    sums = jnp.stack([jnp.sum(local, -1), jnp.sum(local * whitened, -1)])
    norm_grad = lax.psum_scatter(partial, "mp", scatter_dimension=1, tiled=True)
    sums = lax.psum(sums, "mp") * (1.0 / width)
    normed = (whitened * gain_row).astype(BF16)
    micro_index = jnp.arange(row_total, dtype=jnp.int32) // TOK_MB
    live_mask = (micro_index < counts[0]).astype(BF16)
    masked = value_grad[0] * live_mask[:, None]
    product = lax.dot_general(
        masked, normed, (((0,), (0,)), ((), ())), preferred_element_type=F32
    )
    weight_grad = lax.psum_scatter(
        product.astype(BF16), "dp", scatter_dimension=0, tiled=True
    )[None]
    scaled = norm_grad.astype(F32) * cols(gain)
    branch = inv_scale * (scaled - sums[0][:, None] - cols(whitened) * sums[1][:, None])
    above = (cols(top_grad).astype(F32) + branch).astype(BF16)
    below = lax.ppermute(above, "section", [(1, 0)])
    lower = (below.astype(F32) + branch).astype(BF16)
    result = jnp.where(section_index == 0, lower, above)
    return (weight_grad, result[None])


def solution(mesh):
    in_specs = (
        P("section", "dp", "mp"),
        P("section", "dp", None),
        P("section", "mp", None),
        P("section", None),
        P("dp", None),
        P("dp"),
    )
    out_specs = (P("section", ("mp", "dp"), None), P("section", "dp", "mp"))
    grid = (mesh.shape["section"], mesh.shape["mp"], mesh.shape["dp"])
    step = fused if grid == (2, 4, 4) else collectives
    return jax.shard_map(step, mesh=mesh, in_specs=in_specs, out_specs=out_specs, check_vma=False)
```

```python
import functools

import jax
import jax.numpy as jnp
from jax import lax
from jax.experimental import pallas as pl
from jax.experimental.pallas import tpu as pltpu
from jax.sharding import PartitionSpec as P

TOK_MB = 256
LANES = 128
ROWS = 128
LN_ROWS = 64
EPS = 1e-06
F32 = jnp.float32
BF16 = jnp.bfloat16
MESH = pl.DeviceIdType.MESH


def kernel(
    dims,
    vg_hbm,
    st_hbm,
    w_hbm,
    gain_hbm,
    top_hbm,
    counts_ref,
    wg_ref,
    res_ref,
    vg_v,
    st_v,
    w_v,
    top_v,
    gain_ref,
    mean_v,
    inv_v,
    nrm,
    nrm_in,
    vgt,
    vgt_in,
    ssend,
    srecv,
    rt,
    psend,
    precv,
    acc,
    sums,
    sums_in,
    above_in,
    branch_v,
    load_sem,
    n_send,
    n_recv,
    fwd_send,
    vgt_send,
    vgt_recv,
    s_send,
    s_recv,
    rt_send,
    wg_recv,
    p_send,
    p_recv,
    sum_send,
    sum_recv,
    above_send,
    above_recv,
):
    tokens, width, feats, quarter, out_rows = dims
    blocks = width // LANES
    per_quarter = quarter // LANES
    chunks = tokens // ROWS
    sec = lax.axis_index("section")
    m = lax.axis_index("mp")
    z = lax.axis_index("dp")
    inner = lax.rem(z, 3) != 0
    outer = lax.rem(z, 3) == 0
    mate = z + 1 - 2 * lax.rem(z, 2)
    cross = 3 - z
    keep_half = z // 2
    give_half = 1 - z // 2
    own_slot = lax.rem(z, 2)
    mate_slot = 1 - own_slot

    def peer(kk):
        row = lax.rem(m // 2 + kk // 2, 2)
        col = lax.rem(lax.rem(m, 2) + lax.rem(kk, 2), 2)
        return 2 * row + col

    def column(kk, idx):
        return peer(kk) * per_quarter + idx

    def lanes(start, size=LANES):
        return pl.ds(pl.multiple_of(start, LANES), size)

    def row_chunk(i):
        return pl.ds(pl.multiple_of(i * ROWS, ROWS), ROWS)

    def remote(src, dst, send, recv, where):
        return pltpu.make_async_remote_copy(
            src_ref=src,
            dst_ref=dst,
            send_sem=send,
            recv_sem=recv,
            device_id=where,
            device_id_type=MESH,
        )

    load_vg = pltpu.make_async_copy(vg_hbm.at[0], vg_v, load_sem.at[0])
    load_vg.start()
    load_st = pltpu.make_async_copy(st_hbm.at[0], st_v, load_sem.at[1])
    load_st.start()
    load_gain = pltpu.make_async_copy(gain_hbm, gain_ref, load_sem.at[7])
    load_gain.start()

    def load_w(kk):
        return pltpu.make_async_copy(
            w_hbm.at[0, :, lanes(peer(kk) * quarter, quarter)],
            w_v.at[kk],
            load_sem.at[2 + kk],
        )

    for kk in (3, 2, 1, 0):
        load_w(kk).start()
    load_top = pltpu.make_async_copy(
        top_hbm.at[:, lanes(m * quarter, quarter)], top_v, load_sem.at[6]
    )
    load_top.start()

    barrier = pltpu.get_barrier_semaphore()

    def greet(where):
        pl.semaphore_signal(barrier, inc=1, device_id=where, device_id_type=MESH)

    for kk in (1, 2, 3):
        greet({"mp": peer(kk)})
    greet({"dp": mate})
    greet({"section": 1 - sec})

    @pl.when(inner)
    def _():
        greet({"dp": cross})
        pl.semaphore_wait(barrier, 6)

    @pl.when(outer)
    def _():
        pl.semaphore_wait(barrier, 5)

    load_vg.wait()
    half = feats // 2
    for h in range(2):
        vgt[h] = vg_v[:, h * half : (h + 1) * half].T.reshape(2, out_rows, tokens)

    def copy_give():
        return remote(
            vgt.at[give_half],
            vgt_in.at[give_half],
            vgt_send.at[0],
            vgt_recv.at[0],
            {"dp": mate},
        )

    def copy_keep(slot):
        return remote(
            vgt.at[keep_half, slot],
            vgt_in.at[keep_half, slot],
            vgt_send.at[1],
            vgt_recv.at[1],
            {"dp": mate},
        )

    early = jnp.logical_and(outer, sec == 0)
    late = jnp.logical_and(outer, sec == 1)

    @pl.when(early)
    def _():
        copy_give().start()

    load_gain.wait()
    load_st.wait()
    live_count = counts_ref[0]

    def norm_chunk(i, carry):
        first = pl.multiple_of(i * LN_ROWS, LN_ROWS)
        rows = pl.ds(first, LN_ROWS)
        total = jnp.zeros((LN_ROWS, LANES), F32)
        for t in range(blocks):
            total = total + st_v[rows, t * LANES : (t + 1) * LANES].astype(F32)
        mean = jnp.sum(total, axis=-1, keepdims=True) * (1.0 / width)
        mean = jnp.broadcast_to(mean, (LN_ROWS, LANES))
        total = jnp.zeros((LN_ROWS, LANES), F32)
        for t in range(blocks):
            centred = st_v[rows, t * LANES : (t + 1) * LANES].astype(F32) - mean
            total = total + centred * centred
        var = jnp.sum(total, axis=-1, keepdims=True) * (1.0 / width)
        inv = jnp.broadcast_to(lax.rsqrt(var + EPS), (LN_ROWS, LANES))
        mean_v[rows] = mean
        inv_v[rows] = inv
        live = (first // TOK_MB < live_count).astype(F32)
        scale = inv * live
        for t in range(blocks):
            cols = slice(t * LANES, (t + 1) * LANES)
            white = (st_v[rows, cols].astype(F32) - mean) * scale
            nrm[t, rows] = (white * gain_ref[:, cols]).astype(BF16)
        return carry

    lax.fori_loop(0, tokens // LN_ROWS, norm_chunk, 0)

    def copy_normed(kk, idx):
        c = column(kk, idx)
        return remote(
            nrm.at[c], nrm_in.at[c], n_send.at[c], n_recv.at[c], {"dp": mate}
        )

    split = per_quarter - 2

    def send_normed():
        def send_pair(idx, carry):
            copy_normed(0, idx).start()
            copy_normed(3, idx).start()
            return carry

        lax.fori_loop(0, split, send_pair, 0)
        copy_keep(mate_slot).start()
        lax.fori_loop(split, per_quarter, send_pair, 0)

    @pl.when(early)
    def _():
        send_normed()

    upper = chunks // 2
    hold = jnp.logical_and(inner, sec == 0)

    def copy_part(kk, chunk):
        rows = row_chunk(chunk)
        first_hop = 1 + chunk // upper
        hop = jnp.where(kk == 3, first_hop, kk)
        return remote(
            psend.at[kk, rows],
            precv.at[kk, rows],
            p_send.at[kk, chunk],
            p_recv.at[kk, chunk],
            {"mp": peer(hop)},
        )

    def pass_on(chunk):
        rows = row_chunk(chunk)
        kk = 2 - chunk // upper
        copy_part(3, chunk).wait_recv()
        psend[kk, rows] = (psend[kk, rows].astype(F32) + precv[3, rows].astype(F32)).astype(BF16)
        copy_part(kk, chunk).start()

    def pass_all():
        def one(chunk, carry):
            pass_on(chunk)
            return carry

        lax.fori_loop(0, chunks, one, 0)

    acc[...] = jnp.zeros_like(acc)

    def part_step(s, carry):
        kk = 3 - s // chunks
        chunk = lax.rem(s, chunks)
        rows = row_chunk(chunk)
        q = peer(kk)

        @pl.when(chunk == 0)
        def _():
            load_w(kk).wait()

        part = jnp.dot(vg_v[rows], w_v[kk], preferred_element_type=F32).astype(BF16)
        psend[kk, rows] = part
        first = jnp.zeros((ROWS, LANES), F32)
        second = jnp.zeros((ROWS, LANES), F32)
        mean = mean_v[rows]
        inv = inv_v[rows]
        for j in range(per_quarter):
            cols = lanes(q * quarter + j * LANES)
            local = part[:, j * LANES : (j + 1) * LANES].astype(F32) * gain_ref[:, cols]
            white = (st_v[rows, cols].astype(F32) - mean) * inv
            first = first + local
            second = second + local * white
        acc[0, rows] += first
        acc[1, rows] += second

        direct = jnp.logical_or(kk == 3, kk == 1 + chunk // upper)

        @pl.when(jnp.logical_and(direct, jnp.logical_or(outer, sec == 1)))
        def _():
            copy_part(kk, chunk).start()

        return carry

    lax.fori_loop(0, 4 * chunks, part_step, 0)

    @pl.when(late)
    def _():
        copy_give().start()
        send_normed()

    lane = lax.broadcasted_iota(jnp.int32, (tokens, LANES), 1)
    sum0 = jnp.sum(acc[0], axis=-1, keepdims=True)
    sum1 = jnp.sum(acc[1], axis=-1, keepdims=True)
    packed = jnp.where(lane == 0, sum0, jnp.where(lane == 1, sum1, 0.0))
    sums[...] = packed.T[:8]

    def copy_sums(kk):
        return remote(
            sums, sums_in.at[kk], sum_send.at[kk], sum_recv.at[kk], {"mp": peer(kk)}
        )

    for kk in (3, 2, 1):
        copy_sums(kk).start()

    @pl.when(jnp.logical_or(outer, sec == 1))
    def _():
        pass_all()

    def copy_above(chunk):
        rows = row_chunk(chunk)
        return remote(
            res_ref.at[rows],
            above_in.at[rows],
            above_send.at[chunk],
            above_recv.at[chunk],
            {"section": 1 - sec},
        )

    def residual():
        load_top.wait()
        for kk in (1, 2, 3):
            copy_sums(kk).wait_recv()
        total = (sums[...] + sums_in[1]) + (sums_in[2] + sums_in[3])
        total = jnp.concatenate([total] * (LANES // 8), axis=0) * (1.0 / width)
        total = total.T
        acc[0] = jnp.broadcast_to(total[:, 0:1], (tokens, LANES))
        acc[1] = jnp.broadcast_to(total[:, 1:2], (tokens, LANES))

        def rows_step(chunk, carry):
            rows = row_chunk(chunk)
            for kk in (1, 2):
                copy_part(kk, chunk).wait_recv()
            mean = mean_v[rows]
            inv = inv_v[rows]
            for j in range(per_quarter):
                here = slice(j * LANES, (j + 1) * LANES)
                cols = lanes(m * quarter + j * LANES)
                grad = psend[0, rows, here].astype(F32)
                for kk in (1, 2):
                    grad = grad + precv[kk, rows, here].astype(F32)
                scaled = grad * gain_ref[:, cols]
                white = (st_v[rows, cols].astype(F32) - mean) * inv
                branch = inv * (scaled - acc[0, rows] - white * acc[1, rows])
                branch_v[rows, here] = branch
                res_ref[rows, here] = (top_v[rows, here].astype(F32) + branch).astype(
                    BF16
                )

            @pl.when(sec == 1)
            def _():
                copy_above(chunk).start()

            return carry

        lax.fori_loop(0, chunks, rows_step, 0)

    def residual_lower():
        @pl.when(sec == 0)
        def _():
            def lower(chunk, carry):
                rows = row_chunk(chunk)
                copy_above(chunk).wait_recv()
                res_ref[rows] = (above_in[rows].astype(F32) + branch_v[rows]).astype(
                    BF16
                )
                return carry

            lax.fori_loop(0, chunks, lower, 0)

    def copy_wg(c):
        return remote(
            rt.at[0, c],
            rt.at[1, c],
            rt_send.at[c],
            wg_recv.at[c],
            {"dp": mate},
        )

    def column_at(i):
        return column(lax.rem(3 * lax.rem(i, 4), 4), i // 4)

    @pl.when(outer)
    def _():
        residual()
        residual_lower()

        def finish(i, carry):
            c = column_at(i)
            own = jnp.dot(vgt[keep_half, own_slot], nrm[c], preferred_element_type=F32)
            copy_wg(c).wait_recv()
            wg_ref[:, lanes(c * LANES)] = (own + rt[1, c].astype(F32)).astype(BF16)
            return carry

        lax.fori_loop(0, blocks, finish, 0)
        copy_give().wait_send()
        copy_keep(mate_slot).wait_send()

        def sent(idx, carry):
            copy_normed(0, idx).wait_send()
            copy_normed(3, idx).wait_send()
            return carry

        lax.fori_loop(0, per_quarter, sent, 0)

    @pl.when(inner)
    def _():
        def copy_forward(kk, idx):
            c = column(0, idx)
            return remote(
                nrm_in.at[c],
                nrm_in.at[c],
                fwd_send.at[kk - 1, idx],
                n_recv.at[c],
                {"mp": peer(kk)},
            )

        def copy_cross(c):
            return remote(
                ssend.at[c], srecv.at[c], s_send.at[c], s_recv.at[c], {"dp": cross}
            )

        def wait_normed(c):
            remote(
                nrm.at[c], nrm_in.at[c], n_send.at[c], n_recv.at[c], {"dp": mate}
            ).wait_recv()

        def forward(idx):
            wait_normed(column(0, idx))
            copy_forward(1, idx).start()
            copy_forward(2, idx).start()

        def dot(features, rows):
            return jnp.dot(features, rows, preferred_element_type=F32)

        def give(i):
            c = column_at(i)

            @pl.when(lax.rem(i, 4) != 0)
            def _():
                wait_normed(c)

            rows = (2 * out_rows, tokens)
            total = dot(vgt[give_half].reshape(rows), nrm[c])
            total = total + dot(vgt_in[give_half].reshape(rows), nrm_in[c])
            ssend[c] = total.astype(BF16).reshape(2, out_rows, LANES)
            copy_cross(c).start()

            following = i // 4 + 1
            soon = jnp.logical_and(sec == 0, following < split)
            turn = lax.rem(i, 4) == jnp.where(soon, 1, 3)

            @pl.when(jnp.logical_and(turn, following < per_quarter))
            def _():
                forward(following)

            @pl.when(jnp.logical_and(hold, i == 5))
            def _():
                for chunk in range(0, chunks, 2):
                    copy_part(3, chunk).start()

            @pl.when(jnp.logical_and(hold, i == 9))
            def _():
                for chunk in range(1, chunks, 2):
                    copy_part(3, chunk).start()

            @pl.when(jnp.logical_and(hold, i == 12))
            def _():
                for chunk in range(chunks):
                    copy_part(1 + chunk // upper, chunk).start()

            @pl.when(jnp.logical_and(hold, i == 14))
            def _():
                pass_all()

        def keep(i):
            c = column_at(i)
            copy_cross(c).wait_recv()
            theirs = dot(vgt[keep_half, mate_slot], nrm[c])
            rt[0, c] = (theirs + srecv[c, mate_slot].astype(F32)).astype(BF16)
            copy_wg(c).start()
            mine = dot(vgt[keep_half, own_slot], nrm[c])
            mine = mine + dot(vgt_in[keep_half, own_slot], nrm_in[c])
            mine = mine + srecv[c, own_slot].astype(F32)
            wg_ref[:, lanes(c * LANES)] = mine.astype(BF16)

        copy_give().wait_recv()
        forward(0)

        head = 4 * split

        def first(i, carry):
            give(i)
            return carry

        lax.fori_loop(0, head, first, 0)

        @pl.when(sec == 1)
        def _():
            residual()

        copy_keep(own_slot).wait_recv()

        def both(i, carry):
            give(i)
            keep(i - head)
            return carry

        lax.fori_loop(head, blocks, both, 0)

        @pl.when(sec == 0)
        def _():
            residual()

        def last(i, carry):
            keep(i)
            return carry

        lax.fori_loop(blocks - head, blocks, last, 0)
        residual_lower()

        def sent(c, carry):
            copy_cross(c).wait_send()
            copy_wg(c).wait_send()
            return carry

        lax.fori_loop(0, blocks, sent, 0)

        def forwarded(idx, carry):
            copy_forward(1, idx).wait_send()
            copy_forward(2, idx).wait_send()
            return carry

        lax.fori_loop(0, per_quarter, forwarded, 0)

    for kk in (1, 2, 3):
        copy_sums(kk).wait_send()

        def part_sent(chunk, carry):
            copy_part(kk, chunk).wait_send()
            return carry

        lax.fori_loop(0, chunks, part_sent, 0)

    @pl.when(sec == 1)
    def _():
        def above_sent(chunk, carry):
            copy_above(chunk).wait_send()
            return carry

        lax.fori_loop(0, chunks, above_sent, 0)


def fused(value_grad, stream, weights, gain, top_grad, counts):
    tokens, width = stream.shape[1:]
    feats = value_grad.shape[2]
    quarter = width // lax.axis_size("mp")
    out_rows = feats // lax.axis_size("dp")
    blocks = width // LANES
    per_quarter = quarter // LANES
    chunks = tokens // ROWS
    dma = pltpu.SemaphoreType.DMA
    vmem = pltpu.VMEM
    in_hbm = pl.BlockSpec(memory_space=pltpu.HBM)
    in_vmem = pl.BlockSpec(memory_space=pltpu.VMEM)
    weight_grad, residual_grad = pl.pallas_call(
        functools.partial(kernel, (tokens, width, feats, quarter, out_rows)),
        out_shape=(
            jax.ShapeDtypeStruct((out_rows, width), BF16),
            jax.ShapeDtypeStruct((tokens, quarter), BF16),
        ),
        in_specs=[
            in_hbm,
            in_hbm,
            in_hbm,
            in_hbm,
            in_hbm,
            pl.BlockSpec(memory_space=pltpu.SMEM),
        ],
        out_specs=(in_vmem, in_vmem),
        scratch_shapes=[
            vmem((tokens, feats), BF16),
            vmem((tokens, width), BF16),
            vmem((4, feats, quarter), BF16),
            vmem((tokens, quarter), BF16),
            vmem((1, width), F32),
            vmem((tokens, LANES), F32),
            vmem((tokens, LANES), F32),
            vmem((blocks, tokens, LANES), BF16),
            vmem((blocks, tokens, LANES), BF16),
            vmem((2, 2, out_rows, tokens), BF16),
            vmem((2, 2, out_rows, tokens), BF16),
            vmem((blocks, 2, out_rows, LANES), BF16),
            vmem((blocks, 2, out_rows, LANES), BF16),
            vmem((2, blocks, out_rows, LANES), BF16),
            vmem((4, tokens, quarter), BF16),
            vmem((4, tokens, quarter), BF16),
            vmem((2, tokens, LANES), F32),
            vmem((8, tokens), F32),
            vmem((4, 8, tokens), F32),
            vmem((tokens, quarter), BF16),
            vmem((tokens, quarter), F32),
            dma((8,)),
            dma((blocks,)),
            dma((blocks,)),
            dma((2, per_quarter)),
            dma((2,)),
            dma((2,)),
            dma((blocks,)),
            dma((blocks,)),
            dma((blocks,)),
            dma((blocks,)),
            dma((4, chunks)),
            dma((4, chunks)),
            dma((4,)),
            dma((4,)),
            dma((chunks,)),
            dma((chunks,)),
        ],
        compiler_params=pltpu.CompilerParams(
            collective_id=0, has_side_effects=True, vmem_limit_bytes=51 * 2**20
        ),
    )(value_grad, stream, weights, gain, top_grad, counts)
    return weight_grad[None], residual_grad[None]


def normalize(stream_rows):
    values = stream_rows.astype(F32)
    average = jnp.mean(values, axis=-1, keepdims=True)
    centred = values - average
    variance = jnp.mean(centred * centred, axis=-1, keepdims=True)
    inv_scale = lax.rsqrt(variance + EPS)
    return (centred * inv_scale, inv_scale)


def collectives(value_grad, stream, weights, gain, top_grad, counts):
    section_index = lax.axis_index("section")
    model_index = lax.axis_index("mp")
    row_total = stream.shape[1]
    whitened, inv_scale = normalize(stream[0])
    gain_row = gain[0]
    width = whitened.shape[1]
    share = width // lax.axis_size("mp")
    first_col = model_index * share
    cols = lambda a: lax.dynamic_slice_in_dim(a, first_col, share, 1)
    partial = jnp.dot(value_grad[0], weights[0], preferred_element_type=F32)
    partial = partial.astype(BF16)
    local = partial.astype(F32) * gain_row
    sums = jnp.stack([jnp.sum(local, -1), jnp.sum(local * whitened, -1)])
    norm_grad = lax.psum_scatter(partial, "mp", scatter_dimension=1, tiled=True)
    sums = lax.psum(sums, "mp") * (1.0 / width)
    normed = (whitened * gain_row).astype(BF16)
    micro_index = jnp.arange(row_total, dtype=jnp.int32) // TOK_MB
    live_mask = (micro_index < counts[0]).astype(BF16)
    masked = value_grad[0] * live_mask[:, None]
    product = lax.dot_general(
        masked, normed, (((0,), (0,)), ((), ())), preferred_element_type=F32
    )
    weight_grad = lax.psum_scatter(
        product.astype(BF16), "dp", scatter_dimension=0, tiled=True
    )[None]
    scaled = norm_grad.astype(F32) * cols(gain)
    branch = inv_scale * (scaled - sums[0][:, None] - cols(whitened) * sums[1][:, None])
    above = (cols(top_grad).astype(F32) + branch).astype(BF16)
    below = lax.ppermute(above, "section", [(1, 0)])
    lower = (below.astype(F32) + branch).astype(BF16)
    result = jnp.where(section_index == 0, lower, above)
    return (weight_grad, result[None])


def solution(mesh):
    in_specs = (
        P("section", "dp", "mp"),
        P("section", "dp", None),
        P("section", "mp", None),
        P("section", None),
        P("dp", None),
        P("dp"),
    )
    out_specs = (P("section", ("mp", "dp"), None), P("section", "dp", "mp"))
    grid = (mesh.shape["section"], mesh.shape["mp"], mesh.shape["dp"])
    step = fused if grid == (2, 4, 4) else collectives
    return jax.shard_map(step, mesh=mesh, in_specs=in_specs, out_specs=out_specs, check_vma=False)
```

```python
import functools

import jax
import jax.numpy as jnp
from jax import lax
from jax.experimental import pallas as pl
from jax.experimental.pallas import tpu as pltpu
from jax.sharding import PartitionSpec as P

TOK_MB = 256
LANES = 128
ROWS = 128
LN_ROWS = 64
EPS = 1e-06
F32 = jnp.float32
BF16 = jnp.bfloat16
MESH = pl.DeviceIdType.MESH


def kernel(
    dims,
    vg_hbm,
    st_hbm,
    w_hbm,
    gain_hbm,
    top_hbm,
    counts_ref,
    wg_ref,
    res_ref,
    vg_v,
    st_v,
    w_v,
    top_v,
    gain_ref,
    mean_v,
    inv_v,
    nrm,
    nrm_in,
    vgt,
    vgt_in,
    ssend,
    srecv,
    rt,
    psend,
    precv,
    acc,
    sums,
    sums_in,
    above_in,
    branch_v,
    load_sem,
    n_send,
    n_recv,
    fwd_send,
    vgt_send,
    vgt_recv,
    s_send,
    s_recv,
    rt_send,
    wg_recv,
    p_send,
    p_recv,
    sum_send,
    sum_recv,
    above_send,
    above_recv,
):
    tokens, width, feats, quarter, out_rows = dims
    blocks = width // LANES
    per_quarter = quarter // LANES
    chunks = tokens // ROWS
    sec = lax.axis_index("section")
    m = lax.axis_index("mp")
    z = lax.axis_index("dp")
    inner = lax.rem(z, 3) != 0
    outer = lax.rem(z, 3) == 0
    mate = z + 1 - 2 * lax.rem(z, 2)
    cross = 3 - z
    keep_half = z // 2
    give_half = 1 - z // 2
    own_slot = lax.rem(z, 2)
    mate_slot = 1 - own_slot

    def peer(kk):
        row = lax.rem(m // 2 + kk // 2, 2)
        col = lax.rem(lax.rem(m, 2) + lax.rem(kk, 2), 2)
        return 2 * row + col

    def column(kk, idx):
        return peer(kk) * per_quarter + idx

    def lanes(start, size=LANES):
        return pl.ds(pl.multiple_of(start, LANES), size)

    def row_chunk(i):
        return pl.ds(pl.multiple_of(i * ROWS, ROWS), ROWS)

    def remote(src, dst, send, recv, where):
        return pltpu.make_async_remote_copy(
            src_ref=src,
            dst_ref=dst,
            send_sem=send,
            recv_sem=recv,
            device_id=where,
            device_id_type=MESH,
        )

    load_vg = pltpu.make_async_copy(vg_hbm.at[0], vg_v, load_sem.at[0])
    load_vg.start()
    load_st = pltpu.make_async_copy(st_hbm.at[0], st_v, load_sem.at[1])
    load_st.start()
    load_gain = pltpu.make_async_copy(gain_hbm, gain_ref, load_sem.at[7])
    load_gain.start()

    def load_w(kk):
        return pltpu.make_async_copy(
            w_hbm.at[0, :, lanes(peer(kk) * quarter, quarter)],
            w_v.at[kk],
            load_sem.at[2 + kk],
        )

    for kk in (3, 2, 1, 0):
        load_w(kk).start()
    load_top = pltpu.make_async_copy(
        top_hbm.at[:, lanes(m * quarter, quarter)], top_v, load_sem.at[6]
    )
    load_top.start()

    barrier = pltpu.get_barrier_semaphore()

    def greet(where):
        pl.semaphore_signal(barrier, inc=1, device_id=where, device_id_type=MESH)

    for kk in (1, 2, 3):
        greet({"mp": peer(kk)})
    greet({"dp": mate})
    greet({"section": 1 - sec})

    @pl.when(inner)
    def _():
        greet({"dp": cross})
        pl.semaphore_wait(barrier, 6)

    @pl.when(outer)
    def _():
        pl.semaphore_wait(barrier, 5)

    load_vg.wait()
    half = feats // 2
    for h in range(2):
        vgt[h] = vg_v[:, h * half : (h + 1) * half].T.reshape(2, out_rows, tokens)

    def copy_give():
        return remote(
            vgt.at[give_half],
            vgt_in.at[give_half],
            vgt_send.at[0],
            vgt_recv.at[0],
            {"dp": mate},
        )

    def copy_keep(slot):
        return remote(
            vgt.at[keep_half, slot],
            vgt_in.at[keep_half, slot],
            vgt_send.at[1],
            vgt_recv.at[1],
            {"dp": mate},
        )

    early = jnp.logical_and(outer, sec == 0)
    late = jnp.logical_and(outer, sec == 1)

    @pl.when(early)
    def _():
        copy_give().start()

    load_gain.wait()
    load_st.wait()
    live_count = counts_ref[0]

    def norm_chunk(i, carry):
        first = pl.multiple_of(i * LN_ROWS, LN_ROWS)
        rows = pl.ds(first, LN_ROWS)
        total = jnp.zeros((LN_ROWS, LANES), F32)
        for t in range(blocks):
            total = total + st_v[rows, t * LANES : (t + 1) * LANES].astype(F32)
        mean = jnp.sum(total, axis=-1, keepdims=True) * (1.0 / width)
        mean = jnp.broadcast_to(mean, (LN_ROWS, LANES))
        total = jnp.zeros((LN_ROWS, LANES), F32)
        for t in range(blocks):
            centred = st_v[rows, t * LANES : (t + 1) * LANES].astype(F32) - mean
            total = total + centred * centred
        var = jnp.sum(total, axis=-1, keepdims=True) * (1.0 / width)
        inv = jnp.broadcast_to(lax.rsqrt(var + EPS), (LN_ROWS, LANES))
        mean_v[rows] = mean
        inv_v[rows] = inv
        live = (first // TOK_MB < live_count).astype(F32)
        scale = inv * live
        for t in range(blocks):
            cols = slice(t * LANES, (t + 1) * LANES)
            white = (st_v[rows, cols].astype(F32) - mean) * scale
            nrm[t, rows] = (white * gain_ref[:, cols]).astype(BF16)
        return carry

    lax.fori_loop(0, tokens // LN_ROWS, norm_chunk, 0)

    def copy_normed(kk, idx):
        c = column(kk, idx)
        return remote(
            nrm.at[c], nrm_in.at[c], n_send.at[c], n_recv.at[c], {"dp": mate}
        )

    def send_normed(first, last):
        def send_pair(idx, carry):
            copy_normed(0, idx).start()
            copy_normed(3, idx).start()
            return carry

        lax.fori_loop(first, last, send_pair, 0)

    @pl.when(early)
    def _():
        send_normed(0, 3)

    upper = chunks // 2
    lag = 6
    hold = jnp.logical_and(inner, sec == 0)

    def copy_part(kk, chunk):
        rows = row_chunk(chunk)
        first_hop = 1 + chunk // upper
        hop = jnp.where(kk == 3, first_hop, kk)
        return remote(
            psend.at[kk, rows],
            precv.at[kk, rows],
            p_send.at[kk, chunk],
            p_recv.at[kk, chunk],
            {"mp": peer(hop)},
        )

    def pass_on(chunk):
        rows = row_chunk(chunk)
        kk = 2 - chunk // upper
        copy_part(3, chunk).wait_recv()
        psend[kk, rows] = (psend[kk, rows].astype(F32) + precv[3, rows].astype(F32)).astype(BF16)
        copy_part(kk, chunk).start()

    def pass_all():
        def one(chunk, carry):
            pass_on(chunk)
            return carry

        lax.fori_loop(0, chunks, one, 0)

    def column_at(i):
        return column(lax.rem(3 * lax.rem(i, 4), 4), i // 4)

    def copy_wg(c):
        return remote(
            rt.at[0, c],
            rt.at[1, c],
            rt_send.at[c],
            wg_recv.at[c],
            {"dp": mate},
        )

    def copy_forward(kk, idx):
        c = column(0, idx)
        return remote(
            nrm_in.at[c],
            nrm_in.at[c],
            fwd_send.at[kk - 1, idx],
            n_recv.at[c],
            {"mp": peer(kk)},
        )

    def copy_cross(c):
        return remote(
            ssend.at[c], srecv.at[c], s_send.at[c], s_recv.at[c], {"dp": cross}
        )

    def wait_normed(c):
        remote(
            nrm.at[c], nrm_in.at[c], n_send.at[c], n_recv.at[c], {"dp": mate}
        ).wait_recv()

    def forward(idx):
        wait_normed(column(0, idx))
        copy_forward(1, idx).start()
        copy_forward(2, idx).start()

    def dot(features, rows):
        return jnp.dot(features, rows, preferred_element_type=F32)

    def give(i):
        c = column_at(i)

        @pl.when(lax.rem(i, 4) != 0)
        def _():
            wait_normed(c)

        rows = (2 * out_rows, tokens)
        total = dot(vgt[give_half].reshape(rows), nrm[c])
        total = total + dot(vgt_in[give_half].reshape(rows), nrm_in[c])
        ssend[c] = total.astype(BF16).reshape(2, out_rows, LANES)
        copy_cross(c).start()


    def theirs(i):
        c = column_at(i)
        copy_cross(c).wait_recv()
        total = dot(vgt[keep_half, mate_slot], nrm[c])
        rt[0, c] = (total + srecv[c, mate_slot].astype(F32)).astype(BF16)
        copy_wg(c).start()

    def mine(i):
        c = column_at(i)
        total = dot(vgt[keep_half, own_slot], nrm[c])
        total = total + dot(vgt_in[keep_half, own_slot], nrm_in[c])
        total = total + srecv[c, own_slot].astype(F32)
        wg_ref[:, lanes(c * LANES)] = total.astype(BF16)

    acc[...] = jnp.zeros_like(acc)

    def part_step(s, carry):
        kk = 3 - s // chunks
        chunk = lax.rem(s, chunks)
        rows = row_chunk(chunk)
        q = peer(kk)

        @pl.when(chunk == 0)
        def _():
            load_w(kk).wait()

        part = jnp.dot(vg_v[rows], w_v[kk], preferred_element_type=F32).astype(BF16)
        psend[kk, rows] = part
        first = jnp.zeros((ROWS, LANES), F32)
        second = jnp.zeros((ROWS, LANES), F32)
        mean = mean_v[rows]
        inv = inv_v[rows]
        for j in range(per_quarter):
            cols = lanes(q * quarter + j * LANES)
            local = part[:, j * LANES : (j + 1) * LANES].astype(F32) * gain_ref[:, cols]
            white = (st_v[rows, cols].astype(F32) - mean) * inv
            first = first + local
            second = second + local * white
        acc[0, rows] += first
        acc[1, rows] += second

        direct = jnp.logical_or(kk == 3, kk == 1 + chunk // upper)

        ready = jnp.logical_or(outer, jnp.logical_and(sec == 1, kk == 3))

        @pl.when(jnp.logical_and(direct, ready))
        def _():
            copy_part(kk, chunk).start()

        return carry

    lax.fori_loop(0, 2 * chunks, part_step, 0)

    @pl.when(hold)
    def _():
        copy_give().wait_recv()
        forward(0)
        give(0)

    def copy_sums(kk):
        return remote(
            sums, sums_in.at[kk], sum_send.at[kk], sum_recv.at[kk], {"mp": peer(kk)}
        )

    def send_sums():
        lane = lax.broadcasted_iota(jnp.int32, (tokens, LANES), 1)
        sum0 = jnp.sum(acc[0], axis=-1, keepdims=True)
        sum1 = jnp.sum(acc[1], axis=-1, keepdims=True)
        packed = jnp.where(lane == 0, sum0, jnp.where(lane == 1, sum1, 0.0))
        sums[...] = packed.T[:8]
        for kk in (3, 2, 1):
            copy_sums(kk).start()

    @pl.when(jnp.logical_or(outer, sec == 1))
    def _():
        lax.fori_loop(2 * chunks, 4 * chunks, part_step, 0)

    @pl.when(late)
    def _():
        copy_give().start()
        send_normed(0, per_quarter)
        copy_keep(mate_slot).start()

    @pl.when(jnp.logical_or(outer, sec == 1))
    def _():
        send_sums()

    @pl.when(outer)
    def _():
        pass_all()

    @pl.when(early)
    def _():
        send_normed(3, per_quarter)
        copy_keep(mate_slot).start()

    def copy_above(chunk):
        rows = row_chunk(chunk)
        return remote(
            res_ref.at[rows],
            above_in.at[rows],
            above_send.at[chunk],
            above_recv.at[chunk],
            {"section": 1 - sec},
        )

    def residual():
        load_top.wait()
        for kk in (1, 2, 3):
            copy_sums(kk).wait_recv()
        total = (sums[...] + sums_in[1]) + (sums_in[2] + sums_in[3])
        total = jnp.concatenate([total] * (LANES // 8), axis=0) * (1.0 / width)
        total = total.T
        acc[0] = jnp.broadcast_to(total[:, 0:1], (tokens, LANES))
        acc[1] = jnp.broadcast_to(total[:, 1:2], (tokens, LANES))

        def rows_step(chunk, carry):
            rows = row_chunk(chunk)
            for kk in (1, 2):
                copy_part(kk, chunk).wait_recv()
            mean = mean_v[rows]
            inv = inv_v[rows]
            for j in range(per_quarter):
                here = slice(j * LANES, (j + 1) * LANES)
                cols = lanes(m * quarter + j * LANES)
                grad = psend[0, rows, here].astype(F32)
                for kk in (1, 2):
                    grad = grad + precv[kk, rows, here].astype(F32)
                scaled = grad * gain_ref[:, cols]
                white = (st_v[rows, cols].astype(F32) - mean) * inv
                branch = inv * (scaled - acc[0, rows] - white * acc[1, rows])
                branch_v[rows, here] = branch
                res_ref[rows, here] = (top_v[rows, here].astype(F32) + branch).astype(
                    BF16
                )

            @pl.when(sec == 1)
            def _():
                copy_above(chunk).start()

            return carry

        lax.fori_loop(0, chunks, rows_step, 0)

    def residual_lower():
        @pl.when(sec == 0)
        def _():
            def lower(chunk, carry):
                rows = row_chunk(chunk)
                copy_above(chunk).wait_recv()
                res_ref[rows] = (above_in[rows].astype(F32) + branch_v[rows]).astype(
                    BF16
                )
                return carry

            lax.fori_loop(0, chunks, lower, 0)

    @pl.when(outer)
    def _():
        residual()
        residual_lower()

        def finish(i, carry):
            c = column_at(i)
            own = jnp.dot(vgt[keep_half, own_slot], nrm[c], preferred_element_type=F32)
            copy_wg(c).wait_recv()
            wg_ref[:, lanes(c * LANES)] = (own + rt[1, c].astype(F32)).astype(BF16)
            return carry

        lax.fori_loop(0, blocks, finish, 0)
        copy_give().wait_send()
        copy_keep(mate_slot).wait_send()

        def sent(idx, carry):
            copy_normed(0, idx).wait_send()
            copy_normed(3, idx).wait_send()
            return carry

        lax.fori_loop(0, per_quarter, sent, 0)

    @pl.when(inner)
    def _():
        def step(i):
            give(i)
            following = i // 4 + 1
            soon = jnp.logical_and(sec == 0, following == 1)
            turn = lax.rem(i, 4) == jnp.where(soon, 1, 3)

            @pl.when(jnp.logical_and(turn, following < per_quarter))
            def _():
                forward(following)

            @pl.when(jnp.logical_and(hold, i == 5))
            def _():
                for chunk in range(0, chunks, 2):
                    copy_part(3, chunk).start()

            @pl.when(jnp.logical_and(hold, i == 9))
            def _():
                for chunk in range(1, chunks, 2):
                    copy_part(3, chunk).start()

            @pl.when(jnp.logical_and(hold, jnp.logical_and(i >= 6, i < 6 + 2 * chunks)))
            def _():
                part_step(i - 6 + 2 * chunks, 0)

            @pl.when(jnp.logical_and(hold, i == 14))
            def _():
                send_sums()

            @pl.when(jnp.logical_and(hold, i == 15))
            def _():
                for chunk in range(0, chunks, 2):
                    copy_part(1 + chunk // upper, chunk).start()

            @pl.when(jnp.logical_and(hold, i == 19))
            def _():
                for chunk in range(1, chunks, 2):
                    copy_part(1 + chunk // upper, chunk).start()

            @pl.when(jnp.logical_and(hold, i == 20))
            def _():
                pass_all()

            @pl.when(i >= lag)
            def _():
                theirs(i - lag)

            @pl.when(jnp.logical_and(sec == 1, i == 3))
            def _():
                for chunk in range(0, chunks, 2):
                    copy_part(1 + chunk // upper, chunk).start()

            @pl.when(jnp.logical_and(sec == 1, i == 7))
            def _():
                for chunk in range(1, chunks, 2):
                    copy_part(1 + chunk // upper, chunk).start()

            @pl.when(jnp.logical_and(sec == 1, i == 11))
            def _():
                for chunk in range(0, chunks, 2):
                    pass_on(chunk)

            @pl.when(jnp.logical_and(sec == 1, i == 14))
            def _():
                for chunk in range(1, chunks, 2):
                    pass_on(chunk)

            @pl.when(jnp.logical_and(sec == 1, i == 20))
            def _():
                residual()

            first_mine = jnp.where(sec == 0, blocks - 4, blocks - 9)

            @pl.when(i == first_mine)
            def _():
                copy_keep(own_slot).wait_recv()

            @pl.when(jnp.logical_and(i >= first_mine, i < first_mine + 3))
            def _():
                for k in range(4):
                    mine(4 * (i - first_mine) + k)

        @pl.when(sec == 1)
        def _():
            copy_give().wait_recv()
            forward(0)

        def main(i, carry):
            step(i)
            return carry

        lax.fori_loop(1 - sec, blocks, main, 0)

        def last_blocks(i, carry):
            theirs(i)
            for k in range(2):
                mine(2 * i - blocks + k)
            return carry

        lax.fori_loop(blocks - lag, blocks, last_blocks, 0)

        @pl.when(sec == 0)
        def _():
            residual()

        residual_lower()

        def sent(c, carry):
            copy_cross(c).wait_send()
            copy_wg(c).wait_send()
            return carry

        lax.fori_loop(0, blocks, sent, 0)

        def forwarded(idx, carry):
            copy_forward(1, idx).wait_send()
            copy_forward(2, idx).wait_send()
            return carry

        lax.fori_loop(0, per_quarter, forwarded, 0)

    for kk in (1, 2, 3):
        copy_sums(kk).wait_send()

        def part_sent(chunk, carry):
            copy_part(kk, chunk).wait_send()
            return carry

        lax.fori_loop(0, chunks, part_sent, 0)

    @pl.when(sec == 1)
    def _():
        def above_sent(chunk, carry):
            copy_above(chunk).wait_send()
            return carry

        lax.fori_loop(0, chunks, above_sent, 0)


def fused(value_grad, stream, weights, gain, top_grad, counts):
    tokens, width = stream.shape[1:]
    feats = value_grad.shape[2]
    quarter = width // lax.axis_size("mp")
    out_rows = feats // lax.axis_size("dp")
    blocks = width // LANES
    per_quarter = quarter // LANES
    chunks = tokens // ROWS
    dma = pltpu.SemaphoreType.DMA
    vmem = pltpu.VMEM
    in_hbm = pl.BlockSpec(memory_space=pltpu.HBM)
    in_vmem = pl.BlockSpec(memory_space=pltpu.VMEM)
    placed = [
        pltpu.with_memory_space_constraint(a, pltpu.HBM)
        for a in (value_grad, stream, weights, gain, top_grad)
    ]
    weight_grad, residual_grad = pl.pallas_call(
        functools.partial(kernel, (tokens, width, feats, quarter, out_rows)),
        out_shape=(
            jax.ShapeDtypeStruct((out_rows, width), BF16),
            jax.ShapeDtypeStruct((tokens, quarter), BF16),
        ),
        in_specs=[
            in_hbm,
            in_hbm,
            in_hbm,
            in_hbm,
            in_hbm,
            pl.BlockSpec(memory_space=pltpu.SMEM),
        ],
        out_specs=(in_vmem, in_vmem),
        scratch_shapes=[
            vmem((tokens, feats), BF16),
            vmem((tokens, width), BF16),
            vmem((4, feats, quarter), BF16),
            vmem((tokens, quarter), BF16),
            vmem((1, width), F32),
            vmem((tokens, LANES), F32),
            vmem((tokens, LANES), F32),
            vmem((blocks, tokens, LANES), BF16),
            vmem((blocks, tokens, LANES), BF16),
            vmem((2, 2, out_rows, tokens), BF16),
            vmem((2, 2, out_rows, tokens), BF16),
            vmem((blocks, 2, out_rows, LANES), BF16),
            vmem((blocks, 2, out_rows, LANES), BF16),
            vmem((2, blocks, out_rows, LANES), BF16),
            vmem((4, tokens, quarter), BF16),
            vmem((4, tokens, quarter), BF16),
            vmem((2, tokens, LANES), F32),
            vmem((8, tokens), F32),
            vmem((4, 8, tokens), F32),
            vmem((tokens, quarter), BF16),
            vmem((tokens, quarter), F32),
            dma((8,)),
            dma((blocks,)),
            dma((blocks,)),
            dma((2, per_quarter)),
            dma((2,)),
            dma((2,)),
            dma((blocks,)),
            dma((blocks,)),
            dma((blocks,)),
            dma((blocks,)),
            dma((4, chunks)),
            dma((4, chunks)),
            dma((4,)),
            dma((4,)),
            dma((chunks,)),
            dma((chunks,)),
        ],
        compiler_params=pltpu.CompilerParams(
            collective_id=0, has_side_effects=True, vmem_limit_bytes=51 * 2**20
        ),
    )(*placed, counts)
    return weight_grad[None], residual_grad[None]


def normalize(stream_rows):
    values = stream_rows.astype(F32)
    average = jnp.mean(values, axis=-1, keepdims=True)
    centred = values - average
    variance = jnp.mean(centred * centred, axis=-1, keepdims=True)
    inv_scale = lax.rsqrt(variance + EPS)
    return (centred * inv_scale, inv_scale)


def collectives(value_grad, stream, weights, gain, top_grad, counts):
    section_index = lax.axis_index("section")
    model_index = lax.axis_index("mp")
    row_total = stream.shape[1]
    whitened, inv_scale = normalize(stream[0])
    gain_row = gain[0]
    width = whitened.shape[1]
    share = width // lax.axis_size("mp")
    first_col = model_index * share
    cols = lambda a: lax.dynamic_slice_in_dim(a, first_col, share, 1)
    partial = jnp.dot(value_grad[0], weights[0], preferred_element_type=F32)
    partial = partial.astype(BF16)
    local = partial.astype(F32) * gain_row
    sums = jnp.stack([jnp.sum(local, -1), jnp.sum(local * whitened, -1)])
    norm_grad = lax.psum_scatter(partial, "mp", scatter_dimension=1, tiled=True)
    sums = lax.psum(sums, "mp") * (1.0 / width)
    normed = (whitened * gain_row).astype(BF16)
    micro_index = jnp.arange(row_total, dtype=jnp.int32) // TOK_MB
    live_mask = (micro_index < counts[0]).astype(BF16)
    masked = value_grad[0] * live_mask[:, None]
    product = lax.dot_general(
        masked, normed, (((0,), (0,)), ((), ())), preferred_element_type=F32
    )
    weight_grad = lax.psum_scatter(
        product.astype(BF16), "dp", scatter_dimension=0, tiled=True
    )[None]
    scaled = norm_grad.astype(F32) * cols(gain)
    branch = inv_scale * (scaled - sums[0][:, None] - cols(whitened) * sums[1][:, None])
    above = (cols(top_grad).astype(F32) + branch).astype(BF16)
    below = lax.ppermute(above, "section", [(1, 0)])
    lower = (below.astype(F32) + branch).astype(BF16)
    result = jnp.where(section_index == 0, lower, above)
    return (weight_grad, result[None])


def solution(mesh):
    in_specs = (
        P("section", "dp", "mp"),
        P("section", "dp", None),
        P("section", "mp", None),
        P("section", None),
        P("dp", None),
        P("dp"),
    )
    out_specs = (P("section", ("mp", "dp"), None), P("section", "dp", "mp"))
    grid = (mesh.shape["section"], mesh.shape["mp"], mesh.shape["dp"])
    step = fused if grid == (2, 4, 4) else collectives
    return jax.shard_map(step, mesh=mesh, in_specs=in_specs, out_specs=out_specs, check_vma=False)
```

```python
import functools

import jax
import jax.numpy as jnp
from jax import lax
from jax.experimental import pallas as pl
from jax.experimental.pallas import tpu as pltpu
from jax.sharding import PartitionSpec as P

TOK_MB = 256
LANES = 128
ROWS = 128
LN_ROWS = 64
EPS = 1e-06
F32 = jnp.float32
BF16 = jnp.bfloat16
MESH = pl.DeviceIdType.MESH


def kernel(
    dims,
    vg_hbm,
    st_hbm,
    w_hbm,
    gain_hbm,
    top_hbm,
    counts_ref,
    wg_ref,
    res_ref,
    vg_v,
    st_v,
    w_v,
    top_v,
    gain_ref,
    mean_v,
    inv_v,
    nrm,
    nrm_in,
    vgt,
    vgt_in,
    ssend,
    srecv,
    rt,
    psend,
    precv,
    acc,
    sums,
    sums_in,
    above_in,
    branch_v,
    load_sem,
    n_send,
    n_recv,
    fwd_send,
    vgt_send,
    vgt_recv,
    s_send,
    s_recv,
    rt_send,
    wg_recv,
    p_send,
    p_recv,
    sum_send,
    sum_recv,
    above_send,
    above_recv,
):
    tokens, width, feats, quarter, out_rows = dims
    blocks = width // LANES
    per_quarter = quarter // LANES
    chunks = tokens // ROWS
    sec = lax.axis_index("section")
    m = lax.axis_index("mp")
    z = lax.axis_index("dp")
    inner = lax.rem(z, 3) != 0
    outer = lax.rem(z, 3) == 0
    mate = z + 1 - 2 * lax.rem(z, 2)
    cross = 3 - z
    keep_half = z // 2
    give_half = 1 - z // 2
    own_slot = lax.rem(z, 2)
    mate_slot = 1 - own_slot

    def peer(kk):
        row = lax.rem(m // 2 + kk // 2, 2)
        col = lax.rem(lax.rem(m, 2) + lax.rem(kk, 2), 2)
        return 2 * row + col

    def column(kk, idx):
        return peer(kk) * per_quarter + idx

    def lanes(start, size=LANES):
        return pl.ds(pl.multiple_of(start, LANES), size)

    def row_chunk(i):
        return pl.ds(pl.multiple_of(i * ROWS, ROWS), ROWS)

    def remote(src, dst, send, recv, where):
        return pltpu.make_async_remote_copy(
            src_ref=src,
            dst_ref=dst,
            send_sem=send,
            recv_sem=recv,
            device_id=where,
            device_id_type=MESH,
        )

    def sent(src, dst, sem):
        remote(src, dst, sem, vgt_recv.at[0], {"dp": mate}).wait_send()

    load_vg = pltpu.make_async_copy(vg_hbm.at[0], vg_v, load_sem.at[0])
    load_vg.start()
    load_st = pltpu.make_async_copy(st_hbm.at[0], st_v, load_sem.at[1])
    load_st.start()
    load_gain = pltpu.make_async_copy(gain_hbm, gain_ref, load_sem.at[7])
    load_gain.start()

    def load_w(kk):
        return pltpu.make_async_copy(
            w_hbm.at[0, :, lanes(peer(kk) * quarter, quarter)],
            w_v.at[kk],
            load_sem.at[2 + kk],
        )

    for kk in (3, 2, 1, 0):
        load_w(kk).start()
    load_top = pltpu.make_async_copy(
        top_hbm.at[:, lanes(m * quarter, quarter)], top_v, load_sem.at[6]
    )
    load_top.start()

    barrier = pltpu.get_barrier_semaphore()

    def greet(where):
        pl.semaphore_signal(barrier, inc=1, device_id=where, device_id_type=MESH)

    for kk in (1, 2, 3):
        greet({"mp": peer(kk)})
    greet({"dp": mate})
    greet({"section": 1 - sec})

    @pl.when(inner)
    def _():
        greet({"dp": cross})
        pl.semaphore_wait(barrier, 6)

    @pl.when(outer)
    def _():
        pl.semaphore_wait(barrier, 5)

    load_vg.wait()
    half = feats // 2
    for h in range(2):
        vgt[h] = vg_v[:, h * half : (h + 1) * half].T.reshape(2, out_rows, tokens)

    def copy_give():
        return remote(
            vgt.at[give_half],
            vgt_in.at[give_half],
            vgt_send.at[0],
            vgt_recv.at[0],
            {"dp": mate},
        )

    def copy_keep(slot):
        return remote(
            vgt.at[keep_half, slot],
            vgt_in.at[keep_half, slot],
            vgt_send.at[1],
            vgt_recv.at[1],
            {"dp": mate},
        )

    early = jnp.logical_and(outer, sec == 0)
    late = jnp.logical_and(outer, sec == 1)

    @pl.when(early)
    def _():
        copy_give().start()

    load_gain.wait()
    load_st.wait()
    live_count = counts_ref[0]

    def norm_chunk(i, carry):
        first = pl.multiple_of(i * LN_ROWS, LN_ROWS)
        rows = pl.ds(first, LN_ROWS)
        total = jnp.zeros((LN_ROWS, LANES), F32)
        for t in range(blocks):
            total = total + st_v[rows, t * LANES : (t + 1) * LANES].astype(F32)
        mean = jnp.sum(total, axis=-1, keepdims=True) * (1.0 / width)
        mean = jnp.broadcast_to(mean, (LN_ROWS, LANES))
        total = jnp.zeros((LN_ROWS, LANES), F32)
        for t in range(blocks):
            centred = st_v[rows, t * LANES : (t + 1) * LANES].astype(F32) - mean
            total = total + centred * centred
        var = jnp.sum(total, axis=-1, keepdims=True) * (1.0 / width)
        inv = jnp.broadcast_to(lax.rsqrt(var + EPS), (LN_ROWS, LANES))
        mean_v[rows] = mean
        inv_v[rows] = inv
        live = (first // TOK_MB < live_count).astype(F32)
        scale = inv * live
        for t in range(blocks):
            cols = slice(t * LANES, (t + 1) * LANES)
            white = (st_v[rows, cols].astype(F32) - mean) * scale
            nrm[t, rows] = (white * gain_ref[:, cols]).astype(BF16)
        return carry

    lax.fori_loop(0, tokens // LN_ROWS, norm_chunk, 0)

    def copy_normed(kk, idx):
        c = column(kk, idx)
        return remote(
            nrm.at[c], nrm_in.at[c], n_send, n_recv.at[c], {"dp": mate}
        )

    def send_normed(first, last):
        def send_pair(idx, carry):
            copy_normed(0, idx).start()
            copy_normed(3, idx).start()
            return carry

        lax.fori_loop(first, last, send_pair, 0)

    @pl.when(early)
    def _():
        send_normed(0, 3)

    upper = chunks // 2
    lag = 10
    hold = jnp.logical_and(inner, sec == 0)

    def copy_part(kk, chunk):
        rows = row_chunk(chunk)
        first_hop = 1 + chunk // upper
        hop = jnp.where(kk == 3, first_hop, kk)
        return remote(
            psend.at[kk, rows],
            precv.at[kk, rows],
            p_send,
            p_recv.at[kk - 1, chunk],
            {"mp": peer(hop)},
        )

    def pass_on(chunk):
        rows = row_chunk(chunk)
        kk = 2 - chunk // upper
        copy_part(3, chunk).wait_recv()
        psend[kk, rows] = (psend[kk, rows].astype(F32) + precv[3, rows].astype(F32)).astype(BF16)
        copy_part(kk, chunk).start()

    def pass_all():
        def one(chunk, carry):
            pass_on(chunk)
            return carry

        lax.fori_loop(0, chunks, one, 0)

    def source(i):
        opening = (1 - sec) * (1 - jnp.minimum(i // 8, 1))
        late_half = lax.rem(i, 8) // 4
        odd = lax.rem(i, 2)
        kk = opening * ((1 - late_half) * 3 * odd + late_half * (2 - odd))
        kk = kk + (1 - opening) * lax.rem(3 * lax.rem(i, 4), 4)
        idx = opening * (lax.rem(i, 4) // 2) + (1 - opening) * (i // 4)
        return kk, idx

    def column_at(i):
        return column(*source(i))

    def copy_wg(c):
        return remote(
            rt.at[0, c],
            rt.at[1, c],
            rt_send,
            wg_recv.at[c],
            {"dp": mate},
        )

    def copy_forward(kk, idx):
        c = column(0, idx)
        return remote(
            nrm_in.at[c],
            nrm_in.at[c],
            fwd_send,
            n_recv.at[c],
            {"mp": peer(kk)},
        )

    def copy_cross(c):
        return remote(
            ssend.at[c], srecv.at[c], s_send, s_recv.at[c], {"dp": cross}
        )

    def wait_normed(c):
        remote(
            nrm.at[c], nrm_in.at[c], n_send, n_recv.at[c], {"dp": mate}
        ).wait_recv()

    def forward(idx):
        wait_normed(column(0, idx))
        copy_forward(1, idx).start()
        copy_forward(2, idx).start()

    def dot(features, rows):
        return jnp.dot(features, rows, preferred_element_type=F32)

    def give(i):
        c = column_at(i)

        @pl.when(source(i)[0] != 0)
        def _():
            wait_normed(c)

        rows = (2 * out_rows, tokens)
        total = dot(vgt[give_half].reshape(rows), nrm[c])
        total = total + dot(vgt_in[give_half].reshape(rows), nrm_in[c])
        ssend[c] = total.astype(BF16).reshape(2, out_rows, LANES)
        copy_cross(c).start()


    def theirs(i):
        c = column_at(i)
        copy_cross(c).wait_recv()
        total = dot(vgt[keep_half, mate_slot], nrm[c])
        rt[0, c] = (total + srecv[c, mate_slot].astype(F32)).astype(BF16)
        copy_wg(c).start()

    def mine(i):
        c = column_at(i)
        total = dot(vgt[keep_half, own_slot], nrm[c])
        total = total + dot(vgt_in[keep_half, own_slot], nrm_in[c])
        total = total + srecv[c, own_slot].astype(F32)
        wg_ref[:, lanes(c * LANES)] = total.astype(BF16)

    acc[...] = jnp.zeros_like(acc)

    def part_step(s, carry):
        kk = 3 - s // chunks
        chunk = lax.rem(s, chunks)
        rows = row_chunk(chunk)
        q = peer(kk)

        @pl.when(chunk == 0)
        def _():
            load_w(kk).wait()

        part = jnp.dot(vg_v[rows], w_v[kk], preferred_element_type=F32).astype(BF16)
        psend[kk, rows] = part
        first = jnp.zeros((ROWS, LANES), F32)
        second = jnp.zeros((ROWS, LANES), F32)
        mean = mean_v[rows]
        inv = inv_v[rows]
        for j in range(per_quarter):
            cols = lanes(q * quarter + j * LANES)
            local = part[:, j * LANES : (j + 1) * LANES].astype(F32) * gain_ref[:, cols]
            white = (st_v[rows, cols].astype(F32) - mean) * inv
            first = first + local
            second = second + local * white
        acc[0, rows] += first
        acc[1, rows] += second

        direct = jnp.logical_or(kk == 3, kk == 1 + chunk // upper)

        ready = jnp.logical_or(outer, jnp.logical_and(sec == 1, kk == 3))

        @pl.when(jnp.logical_and(direct, ready))
        def _():
            copy_part(kk, chunk).start()

        return carry

    lax.fori_loop(0, 2 * chunks, part_step, 0)

    @pl.when(hold)
    def _():
        copy_give().wait_recv()
        forward(0)
        give(0)

    def copy_sums(kk):
        return remote(
            sums, sums_in.at[kk - 1], sum_send, sum_recv.at[kk - 1], {"mp": peer(kk)}
        )

    def send_sums():
        lane = lax.broadcasted_iota(jnp.int32, (tokens, LANES), 1)
        sum0 = jnp.sum(acc[0], axis=-1, keepdims=True)
        sum1 = jnp.sum(acc[1], axis=-1, keepdims=True)
        packed = jnp.where(lane == 0, sum0, jnp.where(lane == 1, sum1, 0.0))
        sums[...] = packed.T[:8]
        for kk in (3, 2, 1):
            copy_sums(kk).start()

    @pl.when(jnp.logical_or(outer, sec == 1))
    def _():
        lax.fori_loop(2 * chunks, 4 * chunks, part_step, 0)

    @pl.when(jnp.logical_or(outer, sec == 1))
    def _():
        send_sums()

    @pl.when(outer)
    def _():
        pass_all()

    @pl.when(late)
    def _():
        copy_give().start()
        send_normed(0, per_quarter)
        copy_keep(mate_slot).start()

    @pl.when(early)
    def _():
        send_normed(3, per_quarter)
        copy_keep(mate_slot).start()

    def copy_above(chunk):
        rows = row_chunk(chunk)
        return remote(
            res_ref.at[rows],
            above_in.at[rows],
            above_send,
            above_recv.at[chunk],
            {"section": 1 - sec},
        )

    def residual():
        load_top.wait()
        for kk in (1, 2, 3):
            copy_sums(kk).wait_recv()
        total = (sums[...] + sums_in[0]) + (sums_in[1] + sums_in[2])
        total = jnp.concatenate([total] * (LANES // 8), axis=0) * (1.0 / width)
        total = total.T
        acc[0] = jnp.broadcast_to(total[:, 0:1], (tokens, LANES))
        acc[1] = jnp.broadcast_to(total[:, 1:2], (tokens, LANES))

        def rows_step(chunk, carry):
            rows = row_chunk(chunk)
            for kk in (1, 2):
                copy_part(kk, chunk).wait_recv()
            mean = mean_v[rows]
            inv = inv_v[rows]
            for j in range(per_quarter):
                here = slice(j * LANES, (j + 1) * LANES)
                cols = lanes(m * quarter + j * LANES)
                grad = psend[0, rows, here].astype(F32)
                for kk in (1, 2):
                    grad = grad + precv[kk, rows, here].astype(F32)
                scaled = grad * gain_ref[:, cols]
                white = (st_v[rows, cols].astype(F32) - mean) * inv
                branch = inv * (scaled - acc[0, rows] - white * acc[1, rows])
                branch_v[rows, here] = branch
                res_ref[rows, here] = (top_v[rows, here].astype(F32) + branch).astype(
                    BF16
                )

            @pl.when(sec == 1)
            def _():
                copy_above(chunk).start()

            return carry

        lax.fori_loop(0, chunks, rows_step, 0)

    def residual_lower():
        @pl.when(sec == 0)
        def _():
            def lower(chunk, carry):
                rows = row_chunk(chunk)
                copy_above(chunk).wait_recv()
                res_ref[rows] = (above_in[rows].astype(F32) + branch_v[rows]).astype(
                    BF16
                )
                return carry

            lax.fori_loop(0, chunks, lower, 0)

    @pl.when(outer)
    def _():
        residual()
        residual_lower()

        def finish(i, carry):
            c = column_at(i)
            own = jnp.dot(vgt[keep_half, own_slot], nrm[c], preferred_element_type=F32)
            copy_wg(c).wait_recv()
            wg_ref[:, lanes(c * LANES)] = (own + rt[1, c].astype(F32)).astype(BF16)
            return carry

        lax.fori_loop(0, blocks, finish, 0)
        copy_give().wait_send()
        copy_keep(mate_slot).wait_send()

        several = pl.ds(0, 2 * per_quarter)
        sent(nrm.at[several], nrm_in.at[several], n_send)

    @pl.when(inner)
    def _():
        def step(i):
            give(i)
            following = i // 4 + 1
            soon = jnp.where(sec == 0, following <= 2, following >= 3)
            turn = lax.rem(i, 4) == jnp.where(soon, 1, 3)

            @pl.when(jnp.logical_and(turn, following < per_quarter))
            def _():
                forward(following)

            @pl.when(jnp.logical_and(hold, i == 5))
            def _():
                for chunk in range(0, chunks, 2):
                    copy_part(3, chunk).start()

            @pl.when(jnp.logical_and(hold, i == 9))
            def _():
                for chunk in range(1, chunks, 2):
                    copy_part(3, chunk).start()

            @pl.when(jnp.logical_and(hold, jnp.logical_and(i >= 10, i < 10 + 2 * chunks)))
            def _():
                part_step(i - 10 + 2 * chunks, 0)

            @pl.when(jnp.logical_and(hold, i == 18))
            def _():
                send_sums()

            @pl.when(jnp.logical_and(hold, i == 15))
            def _():
                for chunk in range(0, chunks, 2):
                    copy_part(1 + chunk // upper, chunk).start()

            @pl.when(jnp.logical_and(hold, i == 19))
            def _():
                for chunk in range(1, chunks, 2):
                    copy_part(1 + chunk // upper, chunk).start()

            @pl.when(i >= lag)
            def _():
                theirs(i - lag)

            @pl.when(jnp.logical_and(sec == 1, i == 17))
            def _():
                for chunk in range(1, chunks, 2):
                    copy_part(1 + chunk // upper, chunk).start()
                for chunk in range(1, chunks, 2):
                    pass_on(chunk)

            first_mine = jnp.where(sec == 0, blocks - 3, blocks - 8)

            @pl.when(i == first_mine)
            def _():
                copy_keep(own_slot).wait_recv()

            @pl.when(jnp.logical_and(sec == 0, i >= blocks - 3))
            def _():
                for k in range(4):
                    mine(4 * (i - (blocks - 3)) + k)

            @pl.when(
                jnp.logical_and(
                    sec == 1, jnp.logical_and(i >= blocks - 8, i < blocks - 2)
                )
            )
            def _():
                for k in range(2):
                    mine(2 * (i - (blocks - 8)) + k)

        @pl.when(sec == 1)
        def _():
            for chunk in range(0, chunks, 2):
                copy_part(1 + chunk // upper, chunk).start()
            for chunk in range(0, chunks, 2):
                pass_on(chunk)
            copy_give().wait_recv()
            forward(0)

        def main(i, carry):
            step(i)
            return carry

        lax.fori_loop(1 - sec, blocks, main, 0)

        @pl.when(sec == 0)
        def _():
            pass_all()

        @pl.when(sec == 1)
        def _():
            residual()

        def last_blocks(i, carry):
            theirs(i)

            @pl.when(i >= blocks - 6)
            def _():
                for k in range(2):
                    mine(2 * i - blocks + k)

            return carry

        lax.fori_loop(blocks - lag, blocks, last_blocks, 0)

        @pl.when(sec == 0)
        def _():
            residual()

        residual_lower()

        several = pl.ds(0, 2 * per_quarter)
        sent(ssend, srecv, s_send)
        sent(nrm_in.at[several], nrm_in.at[several], fwd_send)
        sent(rt.at[0], rt.at[1], rt_send)

    three = pl.ds(0, 3)
    sent(sums_in, sums_in, sum_send)
    sent(psend.at[three], precv.at[three], p_send)

    @pl.when(sec == 1)
    def _():
        sent(res_ref, above_in, above_send)


def fused(value_grad, stream, weights, gain, top_grad, counts):
    tokens, width = stream.shape[1:]
    feats = value_grad.shape[2]
    quarter = width // lax.axis_size("mp")
    out_rows = feats // lax.axis_size("dp")
    blocks = width // LANES
    per_quarter = quarter // LANES
    chunks = tokens // ROWS
    dma = pltpu.SemaphoreType.DMA
    vmem = pltpu.VMEM
    in_hbm = pl.BlockSpec(memory_space=pltpu.HBM)
    in_vmem = pl.BlockSpec(memory_space=pltpu.VMEM)
    placed = [
        pltpu.with_memory_space_constraint(a, pltpu.HBM)
        for a in (value_grad, stream, weights, gain, top_grad)
    ]
    weight_grad, residual_grad = pl.pallas_call(
        functools.partial(kernel, (tokens, width, feats, quarter, out_rows)),
        out_shape=(
            jax.ShapeDtypeStruct((out_rows, width), BF16),
            jax.ShapeDtypeStruct((tokens, quarter), BF16),
        ),
        in_specs=[
            in_hbm,
            in_hbm,
            in_hbm,
            in_hbm,
            in_hbm,
            pl.BlockSpec(memory_space=pltpu.SMEM),
        ],
        out_specs=(in_vmem, in_vmem),
        scratch_shapes=[
            vmem((tokens, feats), BF16),
            vmem((tokens, width), BF16),
            vmem((4, feats, quarter), BF16),
            vmem((tokens, quarter), BF16),
            vmem((1, width), F32),
            vmem((tokens, LANES), F32),
            vmem((tokens, LANES), F32),
            vmem((blocks, tokens, LANES), BF16),
            vmem((blocks, tokens, LANES), BF16),
            vmem((2, 2, out_rows, tokens), BF16),
            vmem((2, 2, out_rows, tokens), BF16),
            vmem((blocks, 2, out_rows, LANES), BF16),
            vmem((blocks, 2, out_rows, LANES), BF16),
            vmem((2, blocks, out_rows, LANES), BF16),
            vmem((4, tokens, quarter), BF16),
            vmem((4, tokens, quarter), BF16),
            vmem((2, tokens, LANES), F32),
            vmem((8, tokens), F32),
            vmem((3, 8, tokens), F32),
            vmem((tokens, quarter), BF16),
            vmem((tokens, quarter), F32),
            dma((8,)),
            dma,
            dma((blocks,)),
            dma,
            dma((2,)),
            dma((2,)),
            dma,
            dma((blocks,)),
            dma,
            dma((blocks,)),
            dma,
            dma((3, chunks)),
            dma,
            dma((3,)),
            dma,
            dma((chunks,)),
        ],
        compiler_params=pltpu.CompilerParams(
            collective_id=0, has_side_effects=True, vmem_limit_bytes=51 * 2**20
        ),
    )(*placed, counts)
    return weight_grad[None], residual_grad[None]


def normalize(stream_rows):
    values = stream_rows.astype(F32)
    average = jnp.mean(values, axis=-1, keepdims=True)
    centred = values - average
    variance = jnp.mean(centred * centred, axis=-1, keepdims=True)
    inv_scale = lax.rsqrt(variance + EPS)
    return (centred * inv_scale, inv_scale)


def collectives(value_grad, stream, weights, gain, top_grad, counts):
    section_index = lax.axis_index("section")
    model_index = lax.axis_index("mp")
    row_total = stream.shape[1]
    whitened, inv_scale = normalize(stream[0])
    gain_row = gain[0]
    width = whitened.shape[1]
    share = width // lax.axis_size("mp")
    first_col = model_index * share
    cols = lambda a: lax.dynamic_slice_in_dim(a, first_col, share, 1)
    partial = jnp.dot(value_grad[0], weights[0], preferred_element_type=F32)
    partial = partial.astype(BF16)
    local = partial.astype(F32) * gain_row
    sums = jnp.stack([jnp.sum(local, -1), jnp.sum(local * whitened, -1)])
    norm_grad = lax.psum_scatter(partial, "mp", scatter_dimension=1, tiled=True)
    sums = lax.psum(sums, "mp") * (1.0 / width)
    normed = (whitened * gain_row).astype(BF16)
    micro_index = jnp.arange(row_total, dtype=jnp.int32) // TOK_MB
    live_mask = (micro_index < counts[0]).astype(BF16)
    masked = value_grad[0] * live_mask[:, None]
    product = lax.dot_general(
        masked, normed, (((0,), (0,)), ((), ())), preferred_element_type=F32
    )
    weight_grad = lax.psum_scatter(
        product.astype(BF16), "dp", scatter_dimension=0, tiled=True
    )[None]
    scaled = norm_grad.astype(F32) * cols(gain)
    branch = inv_scale * (scaled - sums[0][:, None] - cols(whitened) * sums[1][:, None])
    above = (cols(top_grad).astype(F32) + branch).astype(BF16)
    below = lax.ppermute(above, "section", [(1, 0)])
    lower = (below.astype(F32) + branch).astype(BF16)
    result = jnp.where(section_index == 0, lower, above)
    return (weight_grad, result[None])


def solution(mesh):
    in_specs = (
        P("section", "dp", "mp"),
        P("section", "dp", None),
        P("section", "mp", None),
        P("section", None),
        P("dp", None),
        P("dp"),
    )
    out_specs = (P("section", ("mp", "dp"), None), P("section", "dp", "mp"))
    grid = (mesh.shape["section"], mesh.shape["mp"], mesh.shape["dp"])
    step = fused if grid == (2, 4, 4) else collectives
    return jax.shard_map(step, mesh=mesh, in_specs=in_specs, out_specs=out_specs, check_vma=False)
```

```python
import functools

import jax
import jax.numpy as jnp
from jax import lax
from jax.experimental import pallas as pl
from jax.experimental.pallas import tpu as pltpu
from jax.sharding import PartitionSpec as P

TOK_MB = 256
LANES = 128
ROWS = 128
LN_ROWS = 64
EPS = 1e-06
F32 = jnp.float32
BF16 = jnp.bfloat16
MESH = pl.DeviceIdType.MESH


def kernel(
    dims,
    vg_hbm,
    st_hbm,
    w_hbm,
    gain_hbm,
    top_hbm,
    counts_ref,
    wg_ref,
    res_ref,
    vg_v,
    st_v,
    w_v,
    top_v,
    gain_ref,
    mean_v,
    inv_v,
    nrm,
    nrm_in,
    vgt,
    vgt_in,
    ssend,
    srecv,
    rt,
    psend,
    precv,
    acc,
    sums,
    sums_in,
    above_in,
    branch_v,
    load_sem,
    n_send,
    n_recv,
    fwd_send,
    vgt_send,
    vgt_recv,
    s_send,
    s_recv,
    near_recv,
    rt_send,
    p_send,
    p_recv,
    sum_send,
    sum_recv,
    above_send,
    above_recv,
):
    tokens, width, feats, quarter, out_rows = dims
    blocks = width // LANES
    per_quarter = quarter // LANES
    chunks = tokens // ROWS
    sec = lax.axis_index("section")
    m = lax.axis_index("mp")
    z = lax.axis_index("dp")
    inner = lax.rem(z, 3) != 0
    outer = lax.rem(z, 3) == 0
    mate = z + 1 - 2 * lax.rem(z, 2)
    cross = 3 - z
    keep_half = z // 2
    give_half = 1 - z // 2
    own_slot = lax.rem(z, 2)
    mate_slot = 1 - own_slot

    def peer(kk):
        row = lax.rem(m // 2 + kk // 2, 2)
        col = lax.rem(lax.rem(m, 2) + lax.rem(kk, 2), 2)
        return 2 * row + col

    def column(kk, idx):
        return peer(kk) * per_quarter + idx

    def lanes(start, size=LANES):
        return pl.ds(pl.multiple_of(start, LANES), size)

    def row_chunk(i):
        return pl.ds(pl.multiple_of(i * ROWS, ROWS), ROWS)

    def remote(src, dst, send, recv, where):
        return pltpu.make_async_remote_copy(
            src_ref=src,
            dst_ref=dst,
            send_sem=send,
            recv_sem=recv,
            device_id=where,
            device_id_type=MESH,
        )

    def sent(src, dst, sem):
        remote(src, dst, sem, vgt_recv.at[0], {"dp": mate}).wait_send()

    load_vg = pltpu.make_async_copy(vg_hbm.at[0], vg_v, load_sem.at[0])
    load_vg.start()
    load_st = pltpu.make_async_copy(st_hbm.at[0], st_v, load_sem.at[1])
    load_st.start()
    load_gain = pltpu.make_async_copy(gain_hbm, gain_ref, load_sem.at[4])
    load_gain.start()

    def load_w(kk):
        return pltpu.make_async_copy(
            w_hbm.at[0, :, lanes(peer(kk) * quarter, quarter)],
            w_v.at[kk],
            load_sem.at[2],
        )

    for kk in (3, 2, 1, 0):
        load_w(kk).start()
    load_top = pltpu.make_async_copy(
        top_hbm.at[:, lanes(m * quarter, quarter)], top_v, load_sem.at[3]
    )
    load_top.start()

    barrier = pltpu.get_barrier_semaphore()

    def greet(where):
        pl.semaphore_signal(barrier, inc=1, device_id=where, device_id_type=MESH)

    for kk in (1, 2, 3):
        greet({"mp": peer(kk)})
    greet({"dp": mate})
    greet({"section": 1 - sec})

    @pl.when(inner)
    def _():
        greet({"dp": cross})

    load_vg.wait()
    half = feats // 2
    for h in range(2):
        vgt[h] = vg_v[:, h * half : (h + 1) * half].T.reshape(2, out_rows, tokens)

    @pl.when(inner)
    def _():
        pl.semaphore_wait(barrier, 6)

    @pl.when(outer)
    def _():
        pl.semaphore_wait(barrier, 5)

    def copy_give(slot, which):
        return remote(
            vgt.at[give_half, slot],
            vgt_in.at[give_half, slot],
            vgt_send.at[which],
            vgt_recv.at[which],
            {"dp": mate},
        )

    def copy_keep(slot):
        return remote(
            vgt.at[keep_half, slot],
            vgt_in.at[keep_half, slot],
            vgt_send.at[2],
            vgt_recv.at[2],
            {"dp": mate},
        )

    early = jnp.logical_and(outer, sec == 0)
    late = jnp.logical_and(outer, sec == 1)

    @pl.when(early)
    def _():
        copy_give(mate_slot, 0).start()

    load_gain.wait()
    load_st.wait()
    live_count = counts_ref[0]

    def norm_chunk(i, carry):
        first = pl.multiple_of(i * LN_ROWS, LN_ROWS)
        rows = pl.ds(first, LN_ROWS)
        total = jnp.zeros((LN_ROWS, LANES), F32)
        for t in range(blocks):
            total = total + st_v[rows, t * LANES : (t + 1) * LANES].astype(F32)
        mean = jnp.sum(total, axis=-1, keepdims=True) * (1.0 / width)
        mean = jnp.broadcast_to(mean, (LN_ROWS, LANES))
        total = jnp.zeros((LN_ROWS, LANES), F32)
        for t in range(blocks):
            centred = st_v[rows, t * LANES : (t + 1) * LANES].astype(F32) - mean
            total = total + centred * centred
        var = jnp.sum(total, axis=-1, keepdims=True) * (1.0 / width)
        inv = jnp.broadcast_to(lax.rsqrt(var + EPS), (LN_ROWS, LANES))
        mean_v[rows] = mean
        inv_v[rows] = inv
        live = (first // TOK_MB < live_count).astype(F32)
        scale = inv * live
        for t in range(blocks):
            cols = slice(t * LANES, (t + 1) * LANES)
            white = (st_v[rows, cols].astype(F32) - mean) * scale
            nrm[t, rows] = (white * gain_ref[:, cols]).astype(BF16)
        return carry

    lax.fori_loop(0, tokens // LN_ROWS, norm_chunk, 0)

    def copy_normed(kk, idx):
        c = column(kk, idx)
        return remote(
            nrm.at[c], nrm_in.at[c], n_send, n_recv.at[c], {"dp": mate}
        )

    def send_normed(first, last):
        def send_pair(idx, carry):
            copy_normed(0, idx).start()
            copy_normed(3, idx).start()
            return carry

        lax.fori_loop(first, last, send_pair, 0)

    @pl.when(early)
    def _():
        send_normed(0, 1)
        copy_give(own_slot, 1).start()
        send_normed(1, 3)

    upper = chunks // 2
    lag = 10
    tail = 8
    hold = jnp.logical_and(inner, sec == 0)

    def copy_part(kk, chunk):
        rows = row_chunk(chunk)
        first_hop = 1 + chunk // upper
        hop = jnp.where(kk == 3, first_hop, kk)
        return remote(
            psend.at[kk, rows],
            precv.at[kk, rows],
            p_send,
            p_recv.at[kk - 1, chunk],
            {"mp": peer(hop)},
        )

    def pass_on(chunk):
        rows = row_chunk(chunk)
        kk = 2 - chunk // upper
        copy_part(3, chunk).wait_recv()
        psend[kk, rows] = (psend[kk, rows].astype(F32) + precv[3, rows].astype(F32)).astype(BF16)
        copy_part(kk, chunk).start()

    def pass_all():
        def one(chunk, carry):
            pass_on(chunk)
            return carry

        lax.fori_loop(0, chunks, one, 0)

    def column_at(i):
        return column(lax.rem(3 * lax.rem(i, 4), 4), i // 4)

    def copy_wg(c):
        return remote(
            rt.at[0, c],
            rt.at[1, c],
            rt_send,
            s_recv.at[c],
            {"dp": mate},
        )

    def copy_forward(kk, idx):
        c = column(0, idx)
        return remote(
            nrm_in.at[c],
            nrm_in.at[c],
            fwd_send,
            n_recv.at[c],
            {"mp": peer(kk)},
        )

    def copy_cross(c):
        return remote(
            ssend.at[c], srecv.at[c], s_send, s_recv.at[c], {"dp": cross}
        )

    def copy_far(c):
        return remote(
            ssend.at[c, own_slot],
            srecv.at[c, own_slot],
            s_send,
            s_recv.at[c],
            {"dp": cross},
        )

    def near_slot(i):
        return lax.rem(i + tail, blocks)

    def copy_near(i):
        c = column_at(i)
        return remote(
            ssend.at[c, mate_slot],
            srecv.at[c, mate_slot],
            s_send,
            near_recv.at[near_slot(i)],
            {"dp": cross},
        )

    def wait_far(c):
        remote(
            ssend.at[c, mate_slot],
            srecv.at[c, mate_slot],
            s_send,
            s_recv.at[c],
            {"dp": cross},
        ).wait_recv()

    def wait_near(i):
        c = column_at(i)
        remote(
            ssend.at[c, own_slot],
            srecv.at[c, own_slot],
            s_send,
            near_recv.at[near_slot(i)],
            {"dp": cross},
        ).wait_recv()

    def wait_normed(c):
        remote(
            nrm.at[c], nrm_in.at[c], n_send, n_recv.at[c], {"dp": mate}
        ).wait_recv()

    def forward(idx):
        wait_normed(column(0, idx))
        copy_forward(1, idx).start()
        copy_forward(2, idx).start()

    def dot(features, rows):
        return jnp.dot(features, rows, preferred_element_type=F32)

    def give(i):
        c = column_at(i)

        @pl.when(lax.rem(i, 4) != 0)
        def _():
            wait_normed(c)

        rows = (2 * out_rows, tokens)
        total = dot(vgt[give_half].reshape(rows), nrm[c])
        total = total + dot(vgt_in[give_half].reshape(rows), nrm_in[c])
        ssend[c] = total.astype(BF16).reshape(2, out_rows, LANES)

        @pl.when(i < blocks - tail)
        def _():
            copy_cross(c).start()

        @pl.when(i >= blocks - tail)
        def _():
            copy_far(c).start()

    def give_rows(i, slot):
        c = column_at(i)
        total = dot(vgt[give_half, slot], nrm[c])
        total = total + dot(vgt_in[give_half, slot], nrm_in[c])
        ssend[c, slot] = total.astype(BF16)

    def theirs(i):
        c = column_at(i)

        halves = jnp.logical_or(
            i >= blocks - tail, jnp.logical_and(sec == 0, i < 2)
        )

        @pl.when(jnp.logical_not(halves))
        def _():
            copy_cross(c).wait_recv()

        @pl.when(halves)
        def _():
            wait_far(c)

        @pl.when(jnp.logical_and(sec == 0, i < 2))
        def _():
            wait_near(i)

        total = dot(vgt[keep_half, mate_slot], nrm[c])
        rt[0, c] = (total + srecv[c, mate_slot].astype(F32)).astype(BF16)
        copy_wg(c).start()

    def mine(i):
        c = column_at(i)
        total = dot(vgt[keep_half, own_slot], nrm[c])
        total = total + dot(vgt_in[keep_half, own_slot], nrm_in[c])
        total = total + srecv[c, own_slot].astype(F32)
        wg_ref[:, lanes(c * LANES)] = total.astype(BF16)

    acc[...] = jnp.zeros_like(acc)

    def part_step(s, carry):
        kk = 3 - s // chunks
        chunk = lax.rem(s, chunks)
        rows = row_chunk(chunk)
        q = peer(kk)

        part = jnp.dot(vg_v[rows], w_v[kk], preferred_element_type=F32).astype(BF16)
        psend[kk, rows] = part
        first = jnp.zeros((ROWS, LANES), F32)
        second = jnp.zeros((ROWS, LANES), F32)
        mean = mean_v[rows]
        inv = inv_v[rows]
        for j in range(per_quarter):
            cols = lanes(q * quarter + j * LANES)
            local = part[:, j * LANES : (j + 1) * LANES].astype(F32) * gain_ref[:, cols]
            white = (st_v[rows, cols].astype(F32) - mean) * inv
            first = first + local
            second = second + local * white
        acc[0, rows] += first
        acc[1, rows] += second

        direct = jnp.logical_or(kk == 3, kk == 1 + chunk // upper)

        ready = jnp.logical_or(outer, jnp.logical_and(sec == 1, kk == 3))

        @pl.when(jnp.logical_and(direct, ready))
        def _():
            copy_part(kk, chunk).start()

        return carry

    pltpu.make_async_copy(w_v, w_v, load_sem.at[2]).wait()
    lax.fori_loop(0, 2 * chunks, part_step, 0)

    @pl.when(hold)
    def _():
        copy_give(own_slot, 0).wait_recv()
        forward(0)
        give_rows(0, own_slot)
        copy_far(column_at(0)).start()
        wait_normed(column_at(1))
        give_rows(1, own_slot)
        copy_far(column_at(1)).start()
        copy_give(mate_slot, 1).wait_recv()
        for i in range(2):
            give_rows(i, mate_slot)
            copy_near(i).start()
        forward(1)

    def copy_sums(kk):
        return remote(
            sums, sums_in.at[kk - 1], sum_send, sum_recv, {"mp": peer(kk)}
        )

    def send_sums():
        lane = lax.broadcasted_iota(jnp.int32, (tokens, LANES), 1)
        sum0 = jnp.sum(acc[0], axis=-1, keepdims=True)
        sum1 = jnp.sum(acc[1], axis=-1, keepdims=True)
        packed = jnp.where(lane == 0, sum0, jnp.where(lane == 1, sum1, 0.0))
        sums[...] = packed.T[:8]
        for kk in (3, 2, 1):
            copy_sums(kk).start()

    @pl.when(jnp.logical_or(outer, sec == 1))
    def _():
        lax.fori_loop(2 * chunks, 4 * chunks, part_step, 0)

    @pl.when(jnp.logical_or(outer, sec == 1))
    def _():
        send_sums()

    @pl.when(outer)
    def _():
        pass_all()

    @pl.when(late)
    def _():
        copy_give(mate_slot, 0).start()
        copy_give(own_slot, 1).start()
        send_normed(0, per_quarter)
        copy_keep(mate_slot).start()

    @pl.when(early)
    def _():
        send_normed(3, per_quarter)
        copy_keep(mate_slot).start()

    def copy_above(chunk):
        rows = row_chunk(chunk)
        return remote(
            res_ref.at[rows],
            above_in.at[rows],
            above_send,
            above_recv.at[chunk],
            {"section": 1 - sec},
        )

    def residual():
        load_top.wait()
        remote(sums_in, sums_in, sum_send, sum_recv, {"dp": mate}).wait_recv()
        total = (sums[...] + sums_in[0]) + (sums_in[1] + sums_in[2])
        total = jnp.concatenate([total] * (LANES // 8), axis=0) * (1.0 / width)
        total = total.T
        acc[0] = jnp.broadcast_to(total[:, 0:1], (tokens, LANES))
        acc[1] = jnp.broadcast_to(total[:, 1:2], (tokens, LANES))

        def rows_step(chunk, carry):
            rows = row_chunk(chunk)
            for kk in (1, 2):
                copy_part(kk, chunk).wait_recv()
            mean = mean_v[rows]
            inv = inv_v[rows]
            for j in range(per_quarter):
                here = slice(j * LANES, (j + 1) * LANES)
                cols = lanes(m * quarter + j * LANES)
                grad = psend[0, rows, here].astype(F32)
                for kk in (1, 2):
                    grad = grad + precv[kk, rows, here].astype(F32)
                scaled = grad * gain_ref[:, cols]
                white = (st_v[rows, cols].astype(F32) - mean) * inv
                branch = inv * (scaled - acc[0, rows] - white * acc[1, rows])
                branch_v[rows, here] = branch
                res_ref[rows, here] = (top_v[rows, here].astype(F32) + branch).astype(
                    BF16
                )

            @pl.when(sec == 1)
            def _():
                copy_above(chunk).start()

            return carry

        lax.fori_loop(0, chunks, rows_step, 0)

    def residual_lower():
        @pl.when(sec == 0)
        def _():
            def lower(chunk, carry):
                rows = row_chunk(chunk)
                copy_above(chunk).wait_recv()
                res_ref[rows] = (above_in[rows].astype(F32) + branch_v[rows]).astype(
                    BF16
                )
                return carry

            lax.fori_loop(0, chunks, lower, 0)

    @pl.when(outer)
    def _():
        residual()
        residual_lower()

        def finish(i, carry):
            c = column_at(i)
            own = jnp.dot(vgt[keep_half, own_slot], nrm[c], preferred_element_type=F32)
            copy_wg(c).wait_recv()
            wg_ref[:, lanes(c * LANES)] = (own + rt[1, c].astype(F32)).astype(BF16)
            return carry

        lax.fori_loop(0, blocks, finish, 0)
        copy_give(mate_slot, 0).wait_send()
        copy_give(own_slot, 1).wait_send()
        copy_keep(mate_slot).wait_send()

        several = pl.ds(0, 2 * per_quarter)
        sent(nrm.at[several], nrm_in.at[several], n_send)

    @pl.when(inner)
    def _():
        def step(i):
            give(i)
            following = i // 4 + 1
            soon = jnp.where(sec == 0, following == 2, following >= 3)
            turn = lax.rem(i, 4) == jnp.where(soon, 1, 3)

            turn = jnp.logical_and(turn, jnp.logical_or(sec == 1, following > 1))

            @pl.when(jnp.logical_and(turn, following < per_quarter))
            def _():
                forward(following)

            @pl.when(jnp.logical_and(hold, i == 5))
            def _():
                for chunk in range(0, chunks, 2):
                    copy_part(3, chunk).start()

            @pl.when(jnp.logical_and(hold, i == 9))
            def _():
                for chunk in range(1, chunks, 2):
                    copy_part(3, chunk).start()

            @pl.when(jnp.logical_and(hold, jnp.logical_and(i >= 10, i < 10 + 2 * chunks)))
            def _():
                part_step(i - 10 + 2 * chunks, 0)

            @pl.when(jnp.logical_and(hold, i == 18))
            def _():
                send_sums()

            @pl.when(jnp.logical_and(hold, i == 15))
            def _():
                for chunk in range(0, chunks, 2):
                    copy_part(1 + chunk // upper, chunk).start()

            @pl.when(jnp.logical_and(hold, i == 19))
            def _():
                for chunk in range(1, chunks, 2):
                    copy_part(1 + chunk // upper, chunk).start()

            @pl.when(i >= lag)
            def _():
                theirs(i - lag)

            @pl.when(jnp.logical_and(sec == 1, i == 17))
            def _():
                for chunk in range(1, chunks, 2):
                    copy_part(1 + chunk // upper, chunk).start()
                pass_all()

        @pl.when(sec == 1)
        def _():
            for chunk in range(0, chunks, 2):
                copy_part(1 + chunk // upper, chunk).start()
            copy_give(own_slot, 0).wait_recv()
            copy_give(mate_slot, 1).wait_recv()
            forward(0)

        def main(i, carry):
            step(i)
            return carry

        lax.fori_loop(2 - 2 * sec, blocks, main, 0)

        def send_near(i, carry):
            copy_near(i).start()
            return carry

        lax.fori_loop(blocks - tail, blocks, send_near, 0)

        @pl.when(sec == 0)
        def _():
            pass_all()

        copy_keep(own_slot).wait_recv()

        def last_far(i, carry):
            theirs(i)

            @pl.when(i < blocks - 2)
            def _():
                for k in range(2):
                    mine(2 * (i - (blocks - lag)) + k)

            return carry

        lax.fori_loop(blocks - lag, blocks, last_far, 0)

        @pl.when(sec == 1)
        def _():
            residual()

        def last_near(i, carry):
            wait_near(i)
            mine(i)
            return carry

        lax.fori_loop(blocks - tail, blocks, last_near, 0)

        @pl.when(sec == 0)
        def _():
            residual()

        residual_lower()

        several = pl.ds(0, 2 * per_quarter)
        sent(ssend, srecv, s_send)
        sent(nrm_in.at[several], nrm_in.at[several], fwd_send)
        sent(rt.at[0], rt.at[1], rt_send)

    three = pl.ds(0, 3)
    sent(sums_in, sums_in, sum_send)
    sent(psend.at[three], precv.at[three], p_send)

    @pl.when(sec == 1)
    def _():
        sent(res_ref, above_in, above_send)


def fused(value_grad, stream, weights, gain, top_grad, counts):
    tokens, width = stream.shape[1:]
    feats = value_grad.shape[2]
    quarter = width // lax.axis_size("mp")
    out_rows = feats // lax.axis_size("dp")
    blocks = width // LANES
    per_quarter = quarter // LANES
    chunks = tokens // ROWS
    dma = pltpu.SemaphoreType.DMA
    vmem = pltpu.VMEM
    in_hbm = pl.BlockSpec(memory_space=pltpu.HBM)
    in_vmem = pl.BlockSpec(memory_space=pltpu.VMEM)
    placed = [
        pltpu.with_memory_space_constraint(a, pltpu.HBM)
        for a in (value_grad, stream, weights, gain, top_grad)
    ]
    weight_grad, residual_grad = pl.pallas_call(
        functools.partial(kernel, (tokens, width, feats, quarter, out_rows)),
        out_shape=(
            jax.ShapeDtypeStruct((out_rows, width), BF16),
            jax.ShapeDtypeStruct((tokens, quarter), BF16),
        ),
        in_specs=[
            in_hbm,
            in_hbm,
            in_hbm,
            in_hbm,
            in_hbm,
            pl.BlockSpec(memory_space=pltpu.SMEM),
        ],
        out_specs=(in_vmem, in_vmem),
        scratch_shapes=[
            vmem((tokens, feats), BF16),
            vmem((tokens, width), BF16),
            vmem((4, feats, quarter), BF16),
            vmem((tokens, quarter), BF16),
            vmem((1, width), F32),
            vmem((tokens, LANES), F32),
            vmem((tokens, LANES), F32),
            vmem((blocks, tokens, LANES), BF16),
            vmem((blocks, tokens, LANES), BF16),
            vmem((2, 2, out_rows, tokens), BF16),
            vmem((2, 2, out_rows, tokens), BF16),
            vmem((blocks, 2, out_rows, LANES), BF16),
            vmem((blocks, 2, out_rows, LANES), BF16),
            vmem((2, blocks, out_rows, LANES), BF16),
            vmem((4, tokens, quarter), BF16),
            vmem((4, tokens, quarter), BF16),
            vmem((2, tokens, LANES), F32),
            vmem((8, tokens), F32),
            vmem((3, 8, tokens), F32),
            vmem((tokens, quarter), BF16),
            vmem((tokens, quarter), F32),
            dma((5,)),
            dma,
            dma((blocks,)),
            dma,
            dma((3,)),
            dma((3,)),
            dma,
            dma((blocks,)),
            dma((10,)),
            dma,
            dma,
            dma((3, chunks)),
            dma,
            dma,
            dma,
            dma((chunks,)),
        ],
        compiler_params=pltpu.CompilerParams(
            collective_id=0, has_side_effects=True, vmem_limit_bytes=51 * 2**20
        ),
    )(*placed, counts)
    held = [
        pltpu.with_memory_space_constraint(a, pltpu.VMEM)
        for a in (weight_grad, residual_grad)
    ]
    weight_grad, residual_grad = pl.pallas_call(
        store,
        out_shape=tuple(jax.ShapeDtypeStruct(a.shape, a.dtype) for a in held),
        in_specs=[in_vmem, in_vmem],
        out_specs=(in_hbm, in_hbm),
        scratch_shapes=[dma((4,))],
    )(*held)
    return weight_grad[None], residual_grad[None]


def store(weight_ref, residual_ref, weight_out, residual_out, sem):
    copies = []
    for k, (src, dst) in enumerate(((weight_ref, weight_out), (residual_ref, residual_out))):
        half = src.shape[0] // 2
        for h in range(2):
            rows = pl.ds(h * half, half)
            copies.append(pltpu.make_async_copy(src.at[rows], dst.at[rows], sem.at[2 * k + h]))
    for copy in copies:
        copy.start()
    for copy in copies:
        copy.wait()


def normalize(stream_rows):
    values = stream_rows.astype(F32)
    average = jnp.mean(values, axis=-1, keepdims=True)
    centred = values - average
    variance = jnp.mean(centred * centred, axis=-1, keepdims=True)
    inv_scale = lax.rsqrt(variance + EPS)
    return (centred * inv_scale, inv_scale)


def collectives(value_grad, stream, weights, gain, top_grad, counts):
    section_index = lax.axis_index("section")
    model_index = lax.axis_index("mp")
    row_total = stream.shape[1]
    whitened, inv_scale = normalize(stream[0])
    gain_row = gain[0]
    width = whitened.shape[1]
    share = width // lax.axis_size("mp")
    first_col = model_index * share
    cols = lambda a: lax.dynamic_slice_in_dim(a, first_col, share, 1)
    partial = jnp.dot(value_grad[0], weights[0], preferred_element_type=F32)
    partial = partial.astype(BF16)
    local = partial.astype(F32) * gain_row
    sums = jnp.stack([jnp.sum(local, -1), jnp.sum(local * whitened, -1)])
    norm_grad = lax.psum_scatter(partial, "mp", scatter_dimension=1, tiled=True)
    sums = lax.psum(sums, "mp") * (1.0 / width)
    normed = (whitened * gain_row).astype(BF16)
    micro_index = jnp.arange(row_total, dtype=jnp.int32) // TOK_MB
    live_mask = (micro_index < counts[0]).astype(BF16)
    masked = value_grad[0] * live_mask[:, None]
    product = lax.dot_general(
        masked, normed, (((0,), (0,)), ((), ())), preferred_element_type=F32
    )
    weight_grad = lax.psum_scatter(
        product.astype(BF16), "dp", scatter_dimension=0, tiled=True
    )[None]
    scaled = norm_grad.astype(F32) * cols(gain)
    branch = inv_scale * (scaled - sums[0][:, None] - cols(whitened) * sums[1][:, None])
    above = (cols(top_grad).astype(F32) + branch).astype(BF16)
    below = lax.ppermute(above, "section", [(1, 0)])
    lower = (below.astype(F32) + branch).astype(BF16)
    result = jnp.where(section_index == 0, lower, above)
    return (weight_grad, result[None])


def solution(mesh):
    in_specs = (
        P("section", "dp", "mp"),
        P("section", "dp", None),
        P("section", "mp", None),
        P("section", None),
        P("dp", None),
        P("dp"),
    )
    out_specs = (P("section", ("mp", "dp"), None), P("section", "dp", "mp"))
    grid = (mesh.shape["section"], mesh.shape["mp"], mesh.shape["dp"])
    step = fused if grid == (2, 4, 4) else collectives
    return jax.shard_map(step, mesh=mesh, in_specs=in_specs, out_specs=out_specs, check_vma=False)
```

```python
import functools

import jax
import jax.numpy as jnp
from jax import lax
from jax.experimental import pallas as pl
from jax.experimental.pallas import tpu as pltpu
from jax.sharding import PartitionSpec as P

TOK_MB = 256
LANES = 128
ROWS = 128
LN_ROWS = 128
EPS = 1e-06
F32 = jnp.float32
BF16 = jnp.bfloat16
MESH = pl.DeviceIdType.MESH


def kernel(
    dims,
    vg_hbm,
    st_hbm,
    w_hbm,
    gain_hbm,
    top_hbm,
    counts_ref,
    wg_ref,
    res_ref,
    vg_v,
    st_v,
    w_v,
    top_v,
    gain_ref,
    mean_v,
    inv_v,
    nrm,
    nrm_in,
    vgt,
    vgt_in,
    ssend,
    srecv,
    rt,
    kept,
    psend,
    precv,
    acc,
    sums,
    sums_in,
    above_in,
    branch_v,
    load_sem,
    n_send,
    n_recv,
    fwd_send,
    vgt_send,
    vgt_recv,
    s_send,
    s_recv,
    near_recv,
    rt_send,
    p_send,
    p_recv,
    sum_send,
    sum_recv,
    above_send,
    above_recv,
):
    tokens, width, feats, quarter, out_rows = dims
    blocks = width // LANES
    per_quarter = quarter // LANES
    chunks = tokens // ROWS
    sec = lax.axis_index("section")
    m = lax.axis_index("mp")
    z = lax.axis_index("dp")
    inner = lax.rem(z, 3) != 0
    outer = lax.rem(z, 3) == 0
    mate = z + 1 - 2 * lax.rem(z, 2)
    cross = 3 - z
    keep_half = z // 2
    give_half = 1 - z // 2
    own_slot = lax.rem(z, 2)
    mate_slot = 1 - own_slot

    def peer(kk):
        row = lax.rem(m // 2 + kk // 2, 2)
        col = lax.rem(lax.rem(m, 2) + lax.rem(kk, 2), 2)
        return 2 * row + col

    def column(kk, idx):
        return peer(kk) * per_quarter + idx

    def lanes(start, size=LANES):
        return pl.ds(pl.multiple_of(start, LANES), size)

    def row_chunk(i):
        return pl.ds(pl.multiple_of(i * ROWS, ROWS), ROWS)

    def remote(src, dst, send, recv, where):
        return pltpu.make_async_remote_copy(
            src_ref=src,
            dst_ref=dst,
            send_sem=send,
            recv_sem=recv,
            device_id=where,
            device_id_type=MESH,
        )

    def sent(src, dst, sem):
        remote(src, dst, sem, vgt_recv.at[0], {"dp": mate}).wait_send()

    load_vg = pltpu.make_async_copy(vg_hbm.at[0], vg_v, load_sem.at[0])
    load_vg.start()
    load_st = pltpu.make_async_copy(st_hbm.at[0], st_v, load_sem.at[1])
    load_st.start()
    load_gain = pltpu.make_async_copy(gain_hbm, gain_ref, load_sem.at[4])
    load_gain.start()

    def load_w(kk):
        return pltpu.make_async_copy(
            w_hbm.at[0, :, lanes(peer(kk) * quarter, quarter)],
            w_v.at[kk],
            load_sem.at[2],
        )

    for kk in (3, 2, 1, 0):
        load_w(kk).start()
    load_top = pltpu.make_async_copy(
        top_hbm.at[:, lanes(m * quarter, quarter)], top_v, load_sem.at[3]
    )
    load_top.start()

    barrier = pltpu.get_barrier_semaphore()

    def greet(where):
        pl.semaphore_signal(barrier, inc=1, device_id=where, device_id_type=MESH)

    for kk in (1, 2):
        greet({"mp": peer(kk)})
    greet({"dp": mate})
    greet({"section": 1 - sec})

    @pl.when(inner)
    def _():
        greet({"dp": cross})

    load_vg.wait()
    half = feats // 2
    for h in range(2):
        vgt[h] = vg_v[:, h * half : (h + 1) * half].T.reshape(2, out_rows, tokens)

    @pl.when(inner)
    def _():
        pl.semaphore_wait(barrier, 5)

    @pl.when(outer)
    def _():
        pl.semaphore_wait(barrier, 4)

    def copy_give(slot, which):
        return remote(
            vgt.at[give_half, slot],
            vgt_in.at[give_half, slot],
            vgt_send.at[which],
            vgt_recv.at[which],
            {"dp": mate},
        )

    def copy_keep(slot):
        return remote(
            vgt.at[keep_half, slot],
            vgt_in.at[keep_half, slot],
            vgt_send.at[2],
            vgt_recv.at[2],
            {"dp": mate},
        )

    early = jnp.logical_and(outer, sec == 0)
    late = jnp.logical_and(outer, sec == 1)

    @pl.when(early)
    def _():
        copy_give(mate_slot, 0).start()

    load_gain.wait()
    load_st.wait()
    live_count = counts_ref[0]

    def norm_chunk(i, carry):
        first = pl.multiple_of(i * LN_ROWS, LN_ROWS)
        rows = pl.ds(first, LN_ROWS)
        total = jnp.zeros((LN_ROWS, LANES), F32)
        for t in range(blocks):
            total = total + st_v[rows, t * LANES : (t + 1) * LANES].astype(F32)
        mean = jnp.sum(total, axis=-1, keepdims=True) * (1.0 / width)
        mean = jnp.broadcast_to(mean, (LN_ROWS, LANES))
        total = jnp.zeros((LN_ROWS, LANES), F32)
        for t in range(blocks):
            centred = st_v[rows, t * LANES : (t + 1) * LANES].astype(F32) - mean
            total = total + centred * centred
        var = jnp.sum(total, axis=-1, keepdims=True) * (1.0 / width)
        inv = jnp.broadcast_to(lax.rsqrt(var + EPS), (LN_ROWS, LANES))
        mean_v[rows] = mean
        inv_v[rows] = inv
        live = (first // TOK_MB < live_count).astype(F32)
        scale = inv * live
        for t in range(blocks):
            cols = slice(t * LANES, (t + 1) * LANES)
            white = (st_v[rows, cols].astype(F32) - mean) * scale
            nrm[t, rows] = (white * gain_ref[:, cols]).astype(BF16)
        return carry

    lax.fori_loop(0, tokens // LN_ROWS, norm_chunk, 0)

    def copy_normed(kk, idx):
        c = column(kk, idx)
        return remote(
            nrm.at[c], nrm_in.at[c], n_send, n_recv.at[c], {"dp": mate}
        )

    def send_normed(first, last):
        def send_pair(idx, carry):
            copy_normed(0, idx).start()
            copy_normed(3, idx).start()
            return carry

        lax.fori_loop(first, last, send_pair, 0)

    @pl.when(early)
    def _():
        send_normed(0, 1)
        copy_give(own_slot, 1).start()
        send_normed(1, 3)

    upper = chunks // 2
    lag = 10
    tail = 8
    hold = jnp.logical_and(inner, sec == 0)

    def copy_part(kk, chunk):
        rows = row_chunk(chunk)
        first_hop = 1 + chunk // upper
        hop = jnp.where(kk == 3, first_hop, kk)
        return remote(
            psend.at[kk, rows],
            precv.at[kk, rows],
            p_send,
            p_recv.at[kk - 1, chunk],
            {"mp": peer(hop)},
        )

    def pass_on(chunk):
        rows = row_chunk(chunk)
        kk = 2 - chunk // upper
        copy_part(3, chunk).wait_recv()
        psend[kk, rows] = (psend[kk, rows].astype(F32) + precv[3, rows].astype(F32)).astype(BF16)
        copy_part(kk, chunk).start()

    def copy_sums(step):
        return remote(
            sums.at[step],
            sums_in.at[step],
            sum_send.at[step],
            sum_recv.at[step],
            {"mp": peer(step + 1)},
        )

    def pass_sums():
        copy_sums(0).wait_recv()
        sums[1] = sums[0] + sums_in[0]
        copy_sums(1).start()

    def pass_all():
        def one(chunk, carry):
            pass_on(chunk)
            return carry

        lax.fori_loop(0, chunks, one, 0)

    def column_at(i):
        return column(lax.rem(3 * lax.rem(i, 4), 4), i // 4)

    def copy_wg(c):
        return remote(
            rt.at[0, c],
            rt.at[1, c],
            rt_send,
            s_recv.at[c],
            {"dp": mate},
        )

    def copy_forward(kk, idx):
        c = column(0, idx)
        return remote(
            nrm_in.at[c],
            nrm_in.at[c],
            fwd_send,
            n_recv.at[c],
            {"mp": peer(kk)},
        )

    def copy_cross(c):
        return remote(
            ssend.at[c], srecv.at[c], s_send, s_recv.at[c], {"dp": cross}
        )

    def copy_far(c):
        return remote(
            ssend.at[c, own_slot],
            srecv.at[c, own_slot],
            s_send,
            s_recv.at[c],
            {"dp": cross},
        )

    def near_slot(i):
        return lax.rem(i + tail, blocks)

    def copy_near(i):
        c = column_at(i)
        return remote(
            ssend.at[c, mate_slot],
            srecv.at[c, mate_slot],
            s_send,
            near_recv.at[near_slot(i)],
            {"dp": cross},
        )

    def wait_far(c):
        remote(
            ssend.at[c, mate_slot],
            srecv.at[c, mate_slot],
            s_send,
            s_recv.at[c],
            {"dp": cross},
        ).wait_recv()

    def wait_near(i):
        c = column_at(i)
        remote(
            ssend.at[c, own_slot],
            srecv.at[c, own_slot],
            s_send,
            near_recv.at[near_slot(i)],
            {"dp": cross},
        ).wait_recv()

    def wait_normed(c):
        remote(
            nrm.at[c], nrm_in.at[c], n_send, n_recv.at[c], {"dp": mate}
        ).wait_recv()

    def forward(idx):
        wait_normed(column(0, idx))
        copy_forward(1, idx).start()
        copy_forward(2, idx).start()

    def dot(features, rows):
        return jnp.dot(features, rows, preferred_element_type=F32)

    def give(i):
        c = column_at(i)

        @pl.when(lax.rem(i, 4) != 0)
        def _():
            wait_normed(c)

        rows = (2 * out_rows, tokens)
        total = dot(vgt[give_half].reshape(rows), nrm[c])
        total = total + dot(vgt_in[give_half].reshape(rows), nrm_in[c])
        ssend[c] = total.astype(BF16).reshape(2, out_rows, LANES)

        @pl.when(i < blocks - tail)
        def _():
            copy_cross(c).start()

        @pl.when(i >= blocks - tail)
        def _():
            copy_far(c).start()

    def give_rows(i, slot):
        c = column_at(i)
        total = dot(vgt[give_half, slot], nrm[c])
        total = total + dot(vgt_in[give_half, slot], nrm_in[c])
        ssend[c, slot] = total.astype(BF16)

    def theirs(i):
        c = column_at(i)
        total = dot(vgt[keep_half].reshape(2 * out_rows, tokens), nrm[c])
        kept[c] = total.reshape(2, out_rows, LANES)
        halves = jnp.logical_or(
            i >= blocks - tail, jnp.logical_and(sec == 0, i < 2)
        )

        @pl.when(jnp.logical_not(halves))
        def _():
            copy_cross(c).wait_recv()

        @pl.when(halves)
        def _():
            wait_far(c)

        @pl.when(jnp.logical_and(sec == 0, i < 2))
        def _():
            wait_near(i)

        total = kept[c, mate_slot] + srecv[c, mate_slot].astype(F32)
        rt[0, c] = total.astype(BF16)
        copy_wg(c).start()

    def mine(i, near=False):
        c = column_at(i)
        total = kept[c, own_slot] + dot(vgt_in[keep_half, own_slot], nrm_in[c])
        if near:
            wait_near(i)
        total = total + srecv[c, own_slot].astype(F32)
        wg_ref[:, lanes(c * LANES)] = total.astype(BF16)

    acc[...] = jnp.zeros_like(acc)

    def part_step(s, carry):
        kk = 3 - s // chunks
        chunk = lax.rem(s, chunks)
        rows = row_chunk(chunk)
        q = peer(kk)

        part = jnp.dot(vg_v[rows], w_v[kk], preferred_element_type=F32).astype(BF16)
        psend[kk, rows] = part
        first = jnp.zeros((ROWS, LANES), F32)
        second = jnp.zeros((ROWS, LANES), F32)
        mean = mean_v[rows]
        inv = inv_v[rows]
        for j in range(per_quarter):
            cols = lanes(q * quarter + j * LANES)
            local = part[:, j * LANES : (j + 1) * LANES].astype(F32) * gain_ref[:, cols]
            white = (st_v[rows, cols].astype(F32) - mean) * inv
            first = first + local
            second = second + local * white
        acc[0, rows] += first
        acc[1, rows] += second

        direct = jnp.logical_or(kk == 3, kk == 1 + chunk // upper)

        ready = jnp.logical_or(outer, jnp.logical_and(sec == 1, kk == 3))

        @pl.when(jnp.logical_and(direct, ready))
        def _():
            copy_part(kk, chunk).start()

        return carry

    pltpu.make_async_copy(w_v, w_v, load_sem.at[2]).wait()
    lax.fori_loop(0, 2 * chunks, part_step, 0)

    @pl.when(hold)
    def _():
        copy_give(own_slot, 0).wait_recv()
        forward(0)
        give_rows(0, own_slot)
        copy_far(column_at(0)).start()
        wait_normed(column_at(1))
        give_rows(1, own_slot)
        copy_far(column_at(1)).start()
        copy_give(mate_slot, 1).wait_recv()
        for i in range(2):
            give_rows(i, mate_slot)
            copy_near(i).start()

    def send_sums():
        lane = lax.broadcasted_iota(jnp.int32, (tokens, LANES), 1)
        sum0 = jnp.sum(acc[0], axis=-1, keepdims=True)
        sum1 = jnp.sum(acc[1], axis=-1, keepdims=True)
        packed = jnp.where(lane == 0, sum0, jnp.where(lane == 1, sum1, 0.0))
        sums[0] = packed.T[:8]
        copy_sums(0).start()

    @pl.when(jnp.logical_or(outer, sec == 1))
    def _():
        lax.fori_loop(2 * chunks, 4 * chunks, part_step, 0)

    @pl.when(jnp.logical_or(outer, sec == 1))
    def _():
        send_sums()

    @pl.when(outer)
    def _():
        pass_all()

    @pl.when(late)
    def _():
        copy_give(mate_slot, 0).start()
        copy_give(own_slot, 1).start()
        send_normed(0, per_quarter)
        copy_keep(mate_slot).start()

    @pl.when(early)
    def _():
        send_normed(3, per_quarter)
        copy_keep(mate_slot).start()

    def copy_above(chunk):
        rows = row_chunk(chunk)
        return remote(
            res_ref.at[rows],
            above_in.at[rows],
            above_send,
            above_recv.at[chunk],
            {"section": 1 - sec},
        )

    def residual():
        load_top.wait()
        copy_sums(1).wait_recv()
        total = sums[1] + sums_in[1]
        total = jnp.concatenate([total] * (LANES // 8), axis=0) * (1.0 / width)
        total = total.T
        acc[0] = jnp.broadcast_to(total[:, 0:1], (tokens, LANES))
        acc[1] = jnp.broadcast_to(total[:, 1:2], (tokens, LANES))

        def rows_step(chunk, carry):
            rows = row_chunk(chunk)
            for kk in (1, 2):
                copy_part(kk, chunk).wait_recv()
            mean = mean_v[rows]
            inv = inv_v[rows]
            for j in range(per_quarter):
                here = slice(j * LANES, (j + 1) * LANES)
                cols = lanes(m * quarter + j * LANES)
                grad = psend[0, rows, here].astype(F32)
                for kk in (1, 2):
                    grad = grad + precv[kk, rows, here].astype(F32)
                scaled = grad * gain_ref[:, cols]
                white = (st_v[rows, cols].astype(F32) - mean) * inv
                branch = inv * (scaled - acc[0, rows] - white * acc[1, rows])
                branch_v[rows, here] = branch
                res_ref[rows, here] = (top_v[rows, here].astype(F32) + branch).astype(
                    BF16
                )

            @pl.when(sec == 1)
            def _():
                copy_above(chunk).start()

            return carry

        lax.fori_loop(0, chunks, rows_step, 0)

    def residual_lower():
        @pl.when(sec == 0)
        def _():
            def lower(chunk, carry):
                rows = row_chunk(chunk)
                copy_above(chunk).wait_recv()
                res_ref[rows] = (above_in[rows].astype(F32) + branch_v[rows]).astype(
                    BF16
                )
                return carry

            lax.fori_loop(0, chunks, lower, 0)

    @pl.when(outer)
    def _():
        pass_sums()
        residual()
        residual_lower()

        def finish(i, carry):
            c = column_at(i)
            own = jnp.dot(vgt[keep_half, own_slot], nrm[c], preferred_element_type=F32)
            copy_wg(c).wait_recv()
            wg_ref[:, lanes(c * LANES)] = (own + rt[1, c].astype(F32)).astype(BF16)
            return carry

        lax.fori_loop(0, blocks, finish, 0)
        copy_give(mate_slot, 0).wait_send()
        copy_give(own_slot, 1).wait_send()
        copy_keep(mate_slot).wait_send()

        several = pl.ds(0, 2 * per_quarter)
        sent(nrm.at[several], nrm_in.at[several], n_send)

    @pl.when(inner)
    def _():
        def step(i):
            give(i)
            following = i // 4 + 1
            soon = jnp.where(sec == 0, following == 2, following >= 3)
            usual = jnp.where(jnp.logical_and(sec == 0, following == 1), 2, 3)
            turn = lax.rem(i, 4) == jnp.where(soon, 1, usual)

            @pl.when(jnp.logical_and(turn, following < per_quarter))
            def _():
                forward(following)

            @pl.when(jnp.logical_and(hold, i == 5))
            def _():
                for chunk in range(0, chunks, 2):
                    copy_part(3, chunk).start()

            @pl.when(jnp.logical_and(hold, i == 9))
            def _():
                for chunk in range(1, chunks, 2):
                    copy_part(3, chunk).start()

            @pl.when(jnp.logical_and(hold, jnp.logical_and(i >= 10, i < 10 + 2 * chunks)))
            def _():
                part_step(i - 10 + 2 * chunks, 0)

            @pl.when(jnp.logical_and(hold, i == 18))
            def _():
                send_sums()

            @pl.when(jnp.logical_and(hold, i == 15))
            def _():
                for chunk in range(0, chunks, 2):
                    copy_part(1 + chunk // upper, chunk).start()

            @pl.when(jnp.logical_and(hold, i == 19))
            def _():
                for chunk in range(1, chunks, 2):
                    copy_part(1 + chunk // upper, chunk).start()

            @pl.when(i >= lag)
            def _():
                theirs(i - lag)

            @pl.when(jnp.logical_and(sec == 1, i == 17))
            def _():
                for chunk in range(chunks):
                    copy_part(1 + chunk // upper, chunk).start()
                pass_sums()
                pass_all()

        @pl.when(sec == 1)
        def _():
            copy_give(own_slot, 0).wait_recv()
            copy_give(mate_slot, 1).wait_recv()
            forward(0)

        def main(i, carry):
            step(i)
            return carry

        lax.fori_loop(2 - 2 * sec, blocks, main, 0)

        def send_near(i, carry):
            copy_near(i).start()
            return carry

        lax.fori_loop(blocks - tail, blocks, send_near, 0)

        @pl.when(sec == 0)
        def _():
            pass_sums()
            pass_all()

        copy_keep(own_slot).wait_recv()

        def last_far(i, carry):
            theirs(i)

            @pl.when(i < blocks - 2)
            def _():
                for k in range(2):
                    mine(2 * (i - (blocks - lag)) + k)

            return carry

        lax.fori_loop(blocks - lag, blocks, last_far, 0)

        @pl.when(sec == 1)
        def _():
            residual()

        def last_near(i, carry):
            mine(i, near=True)
            return carry

        lax.fori_loop(blocks - tail, blocks, last_near, 0)

        @pl.when(sec == 0)
        def _():
            residual()

        residual_lower()

        several = pl.ds(0, 2 * per_quarter)
        sent(ssend, srecv, s_send)
        sent(nrm_in.at[several], nrm_in.at[several], fwd_send)
        sent(rt.at[0], rt.at[1], rt_send)

    three = pl.ds(0, 3)
    for step in range(2):
        copy_sums(step).wait_send()
    sent(psend.at[three], precv.at[three], p_send)

    @pl.when(sec == 1)
    def _():
        sent(res_ref, above_in, above_send)


def fused(value_grad, stream, weights, gain, top_grad, counts):
    tokens, width = stream.shape[1:]
    feats = value_grad.shape[2]
    quarter = width // lax.axis_size("mp")
    out_rows = feats // lax.axis_size("dp")
    blocks = width // LANES
    per_quarter = quarter // LANES
    chunks = tokens // ROWS
    dma = pltpu.SemaphoreType.DMA
    vmem = pltpu.VMEM
    in_hbm = pl.BlockSpec(memory_space=pltpu.HBM)
    in_vmem = pl.BlockSpec(memory_space=pltpu.VMEM)
    placed = [
        pltpu.with_memory_space_constraint(a, pltpu.HBM)
        for a in (value_grad, stream, weights, gain, top_grad)
    ]
    weight_grad, residual_grad = pl.pallas_call(
        functools.partial(kernel, (tokens, width, feats, quarter, out_rows)),
        out_shape=(
            jax.ShapeDtypeStruct((out_rows, width), BF16),
            jax.ShapeDtypeStruct((tokens, quarter), BF16),
        ),
        in_specs=[
            in_hbm,
            in_hbm,
            in_hbm,
            in_hbm,
            in_hbm,
            pl.BlockSpec(memory_space=pltpu.SMEM),
        ],
        out_specs=(in_vmem, in_vmem),
        scratch_shapes=[
            vmem((tokens, feats), BF16),
            vmem((tokens, width), BF16),
            vmem((4, feats, quarter), BF16),
            vmem((tokens, quarter), BF16),
            vmem((1, width), F32),
            vmem((tokens, LANES), F32),
            vmem((tokens, LANES), F32),
            vmem((blocks, tokens, LANES), BF16),
            vmem((blocks, tokens, LANES), BF16),
            vmem((2, 2, out_rows, tokens), BF16),
            vmem((2, 2, out_rows, tokens), BF16),
            vmem((blocks, 2, out_rows, LANES), BF16),
            vmem((blocks, 2, out_rows, LANES), BF16),
            vmem((2, blocks, out_rows, LANES), BF16),
            vmem((blocks, 2, out_rows, LANES), F32),
            vmem((4, tokens, quarter), BF16),
            vmem((4, tokens, quarter), BF16),
            vmem((2, tokens, LANES), F32),
            vmem((2, 8, tokens), F32),
            vmem((2, 8, tokens), F32),
            vmem((tokens, quarter), BF16),
            vmem((tokens, quarter), F32),
            dma((5,)),
            dma,
            dma((blocks,)),
            dma,
            dma((3,)),
            dma((3,)),
            dma,
            dma((blocks,)),
            dma((10,)),
            dma,
            dma,
            dma((3, chunks)),
            dma((2,)),
            dma((2,)),
            dma,
            dma((chunks,)),
        ],
        compiler_params=pltpu.CompilerParams(
            collective_id=0, has_side_effects=True, vmem_limit_bytes=51 * 2**20
        ),
    )(*placed, counts)
    held = [
        pltpu.with_memory_space_constraint(a, pltpu.VMEM)
        for a in (weight_grad, residual_grad)
    ]
    weight_grad, residual_grad = pl.pallas_call(
        store,
        out_shape=tuple(jax.ShapeDtypeStruct(a.shape, a.dtype) for a in held),
        in_specs=[in_vmem, in_vmem],
        out_specs=(in_hbm, in_hbm),
        scratch_shapes=[dma((4,))],
    )(*held)
    return weight_grad[None], residual_grad[None]


def store(weight_ref, residual_ref, weight_out, residual_out, sem):
    copies = []
    for k, (src, dst) in enumerate(((weight_ref, weight_out), (residual_ref, residual_out))):
        half = src.shape[0] // 2
        for h in range(2):
            rows = pl.ds(h * half, half)
            copies.append(pltpu.make_async_copy(src.at[rows], dst.at[rows], sem.at[2 * k + h]))
    for copy in copies:
        copy.start()
    for copy in copies:
        copy.wait()


def normalize(stream_rows):
    values = stream_rows.astype(F32)
    average = jnp.mean(values, axis=-1, keepdims=True)
    centred = values - average
    variance = jnp.mean(centred * centred, axis=-1, keepdims=True)
    inv_scale = lax.rsqrt(variance + EPS)
    return (centred * inv_scale, inv_scale)


def collectives(value_grad, stream, weights, gain, top_grad, counts):
    section_index = lax.axis_index("section")
    model_index = lax.axis_index("mp")
    row_total = stream.shape[1]
    whitened, inv_scale = normalize(stream[0])
    gain_row = gain[0]
    width = whitened.shape[1]
    share = width // lax.axis_size("mp")
    first_col = model_index * share
    cols = lambda a: lax.dynamic_slice_in_dim(a, first_col, share, 1)
    partial = jnp.dot(value_grad[0], weights[0], preferred_element_type=F32)
    partial = partial.astype(BF16)
    local = partial.astype(F32) * gain_row
    sums = jnp.stack([jnp.sum(local, -1), jnp.sum(local * whitened, -1)])
    norm_grad = lax.psum_scatter(partial, "mp", scatter_dimension=1, tiled=True)
    sums = lax.psum(sums, "mp") * (1.0 / width)
    normed = (whitened * gain_row).astype(BF16)
    micro_index = jnp.arange(row_total, dtype=jnp.int32) // TOK_MB
    live_mask = (micro_index < counts[0]).astype(BF16)
    masked = value_grad[0] * live_mask[:, None]
    product = lax.dot_general(
        masked, normed, (((0,), (0,)), ((), ())), preferred_element_type=F32
    )
    weight_grad = lax.psum_scatter(
        product.astype(BF16), "dp", scatter_dimension=0, tiled=True
    )[None]
    scaled = norm_grad.astype(F32) * cols(gain)
    branch = inv_scale * (scaled - sums[0][:, None] - cols(whitened) * sums[1][:, None])
    above = (cols(top_grad).astype(F32) + branch).astype(BF16)
    below = lax.ppermute(above, "section", [(1, 0)])
    lower = (below.astype(F32) + branch).astype(BF16)
    result = jnp.where(section_index == 0, lower, above)
    return (weight_grad, result[None])


def solution(mesh):
    in_specs = (
        P("section", "dp", "mp"),
        P("section", "dp", None),
        P("section", "mp", None),
        P("section", None),
        P("dp", None),
        P("dp"),
    )
    out_specs = (P("section", ("mp", "dp"), None), P("section", "dp", "mp"))
    grid = (mesh.shape["section"], mesh.shape["mp"], mesh.shape["dp"])
    step = fused if grid == (2, 4, 4) else collectives
    return jax.shard_map(step, mesh=mesh, in_specs=in_specs, out_specs=out_specs, check_vma=False)
```

```python
import functools

import jax
import jax.numpy as jnp
from jax import lax
from jax.experimental import pallas as pl
from jax.experimental.pallas import tpu as pltpu
from jax.sharding import PartitionSpec as P

TOK_MB = 256
LANES = 128
ROWS = 128
LN_ROWS = 128
EPS = 1e-06
F32 = jnp.float32
BF16 = jnp.bfloat16
MESH = pl.DeviceIdType.MESH


def kernel(
    dims,
    vg_hbm,
    st_hbm,
    w_hbm,
    gain_hbm,
    top_hbm,
    counts_ref,
    wg_ref,
    res_ref,
    vg_v,
    st_v,
    w_v,
    top_v,
    gain_ref,
    mean_v,
    inv_v,
    nrm,
    nrm_in,
    vgt,
    vgt_in,
    ssend,
    srecv,
    rt,
    kept,
    psend,
    precv,
    acc,
    sums,
    sums_in,
    above_in,
    branch_v,
    load_sem,
    n_send,
    n_recv,
    fwd_send,
    vgt_send,
    vgt_recv,
    s_send,
    s_recv,
    near_recv,
    rt_send,
    p_send,
    p_recv,
    sum_send,
    sum_recv,
    above_send,
    above_recv,
):
    tokens, width, feats, quarter, out_rows = dims
    blocks = width // LANES
    per_quarter = quarter // LANES
    chunks = tokens // ROWS
    sec = lax.axis_index("section")
    m = lax.axis_index("mp")
    z = lax.axis_index("dp")
    inner = lax.rem(z, 3) != 0
    outer = lax.rem(z, 3) == 0
    mate = z + 1 - 2 * lax.rem(z, 2)
    cross = 3 - z
    keep_half = z // 2
    give_half = 1 - z // 2
    own_slot = lax.rem(z, 2)
    mate_slot = 1 - own_slot

    def peer(kk):
        row = lax.rem(m // 2 + kk // 2, 2)
        col = lax.rem(lax.rem(m, 2) + lax.rem(kk, 2), 2)
        return 2 * row + col

    def column(kk, idx):
        return peer(kk) * per_quarter + idx

    def lanes(start, size=LANES):
        return pl.ds(pl.multiple_of(start, LANES), size)

    def row_chunk(i):
        return pl.ds(pl.multiple_of(i * ROWS, ROWS), ROWS)

    def remote(src, dst, send, recv, where):
        return pltpu.make_async_remote_copy(
            src_ref=src,
            dst_ref=dst,
            send_sem=send,
            recv_sem=recv,
            device_id=where,
            device_id_type=MESH,
        )

    def sent(src, dst, sem):
        remote(src, dst, sem, vgt_recv.at[0], {"dp": mate}).wait_send()

    load_vg = pltpu.make_async_copy(vg_hbm.at[0], vg_v, load_sem.at[0])
    load_vg.start()
    load_st = pltpu.make_async_copy(st_hbm.at[0], st_v, load_sem.at[1])
    load_st.start()
    load_gain = pltpu.make_async_copy(gain_hbm, gain_ref, load_sem.at[4])
    load_gain.start()

    def load_w(kk):
        return pltpu.make_async_copy(
            w_hbm.at[0, :, lanes(peer(kk) * quarter, quarter)],
            w_v.at[kk],
            load_sem.at[2],
        )

    for kk in (3, 2, 1, 0):
        load_w(kk).start()
    load_top = pltpu.make_async_copy(
        top_hbm.at[:, lanes(m * quarter, quarter)], top_v, load_sem.at[3]
    )
    load_top.start()

    barrier = pltpu.get_barrier_semaphore()

    def greet(where):
        pl.semaphore_signal(barrier, inc=1, device_id=where, device_id_type=MESH)

    for kk in (1, 2):
        greet({"mp": peer(kk)})
    greet({"dp": mate})
    greet({"section": 1 - sec})

    @pl.when(inner)
    def _():
        greet({"dp": cross})

    load_vg.wait()
    half = feats // 2
    for h in range(2):
        vgt[h] = vg_v[:, h * half : (h + 1) * half].T.reshape(2, out_rows, tokens)

    @pl.when(inner)
    def _():
        pl.semaphore_wait(barrier, 5)

    @pl.when(outer)
    def _():
        pl.semaphore_wait(barrier, 4)

    def copy_give(slot, which):
        return remote(
            vgt.at[give_half, slot],
            vgt_in.at[give_half, slot],
            vgt_send.at[which],
            vgt_recv.at[which],
            {"dp": mate},
        )

    def copy_keep(slot):
        return remote(
            vgt.at[keep_half, slot],
            vgt_in.at[keep_half, slot],
            vgt_send.at[2],
            vgt_recv.at[2],
            {"dp": mate},
        )

    early = jnp.logical_and(outer, sec == 0)
    late = jnp.logical_and(outer, sec == 1)

    @pl.when(early)
    def _():
        copy_give(mate_slot, 0).start()

    load_gain.wait()
    load_st.wait()
    live_count = counts_ref[0]

    def norm_chunk(i, carry):
        first = pl.multiple_of(i * LN_ROWS, LN_ROWS)
        rows = pl.ds(first, LN_ROWS)
        total = jnp.zeros((LN_ROWS, LANES), F32)
        for t in range(blocks):
            total = total + st_v[rows, t * LANES : (t + 1) * LANES].astype(F32)
        mean = jnp.sum(total, axis=-1, keepdims=True) * (1.0 / width)
        mean = jnp.broadcast_to(mean, (LN_ROWS, LANES))
        total = jnp.zeros((LN_ROWS, LANES), F32)
        for t in range(blocks):
            centred = st_v[rows, t * LANES : (t + 1) * LANES].astype(F32) - mean
            total = total + centred * centred
        var = jnp.sum(total, axis=-1, keepdims=True) * (1.0 / width)
        inv = jnp.broadcast_to(lax.rsqrt(var + EPS), (LN_ROWS, LANES))
        mean_v[rows] = mean
        inv_v[rows] = inv
        live = (first // TOK_MB < live_count).astype(F32)
        scale = inv * live
        for t in range(blocks):
            cols = slice(t * LANES, (t + 1) * LANES)
            white = (st_v[rows, cols].astype(F32) - mean) * scale
            nrm[t, rows] = (white * gain_ref[:, cols]).astype(BF16)
        return carry

    lax.fori_loop(0, tokens // LN_ROWS, norm_chunk, 0)

    def copy_normed(kk, idx):
        c = column(kk, idx)
        return remote(
            nrm.at[c], nrm_in.at[c], n_send, n_recv.at[c], {"dp": mate}
        )

    def send_normed(first, last):
        def send_pair(idx, carry):
            copy_normed(0, idx).start()
            copy_normed(3, idx).start()
            return carry

        lax.fori_loop(first, last, send_pair, 0)

    @pl.when(early)
    def _():
        send_normed(0, 1)
        copy_give(own_slot, 1).start()
        send_normed(1, 3)

    upper = chunks // 2
    lag = 10
    tail = 8
    hold = jnp.logical_and(inner, sec == 0)

    def copy_part(kk, chunk):
        rows = row_chunk(chunk)
        first_hop = 1 + chunk // upper
        hop = jnp.where(kk == 3, first_hop, kk)
        return remote(
            psend.at[kk, rows],
            precv.at[kk, rows],
            p_send,
            p_recv.at[kk - 1, chunk],
            {"mp": peer(hop)},
        )

    def pass_on(chunk):
        rows = row_chunk(chunk)
        kk = 2 - chunk // upper
        copy_part(3, chunk).wait_recv()
        psend[kk, rows] = (psend[kk, rows].astype(F32) + precv[3, rows].astype(F32)).astype(BF16)
        copy_part(kk, chunk).start()

    def copy_sums(step):
        return remote(
            sums.at[step],
            sums_in.at[step],
            sum_send.at[step],
            sum_recv.at[step],
            {"mp": peer(step + 1)},
        )

    def pass_sums():
        copy_sums(0).wait_recv()
        sums[1] = sums[0] + sums_in[0]
        copy_sums(1).start()

    def pass_all():
        def one(chunk, carry):
            pass_on(chunk)
            return carry

        lax.fori_loop(0, chunks, one, 0)

    def column_at(i):
        return column(lax.rem(3 * lax.rem(i, 4), 4), i // 4)

    def copy_wg(c):
        return remote(
            rt.at[0, c],
            rt.at[1, c],
            rt_send,
            s_recv.at[c],
            {"dp": mate},
        )

    def copy_forward(kk, idx):
        c = column(0, idx)
        return remote(
            nrm_in.at[c],
            nrm_in.at[c],
            fwd_send,
            n_recv.at[c],
            {"mp": peer(kk)},
        )

    def copy_cross(c):
        return remote(
            ssend.at[c], srecv.at[c], s_send, s_recv.at[c], {"dp": cross}
        )

    def copy_far(c):
        return remote(
            ssend.at[c, own_slot],
            srecv.at[c, own_slot],
            s_send,
            s_recv.at[c],
            {"dp": cross},
        )

    def near_slot(i):
        return lax.rem(i + tail, blocks)

    def copy_near(i):
        c = column_at(i)
        return remote(
            ssend.at[c, mate_slot],
            srecv.at[c, mate_slot],
            s_send,
            near_recv.at[near_slot(i)],
            {"dp": cross},
        )

    def wait_far(c):
        remote(
            ssend.at[c, mate_slot],
            srecv.at[c, mate_slot],
            s_send,
            s_recv.at[c],
            {"dp": cross},
        ).wait_recv()

    def wait_near(i):
        c = column_at(i)
        remote(
            ssend.at[c, own_slot],
            srecv.at[c, own_slot],
            s_send,
            near_recv.at[near_slot(i)],
            {"dp": cross},
        ).wait_recv()

    def wait_normed(c):
        remote(
            nrm.at[c], nrm_in.at[c], n_send, n_recv.at[c], {"dp": mate}
        ).wait_recv()

    def forward(idx):
        wait_normed(column(0, idx))
        copy_forward(1, idx).start()
        copy_forward(2, idx).start()

    def dot(features, rows):
        return jnp.dot(features, rows, preferred_element_type=F32)

    def give(i):
        c = column_at(i)

        @pl.when(lax.rem(i, 4) != 0)
        def _():
            wait_normed(c)

        rows = (2 * out_rows, tokens)
        total = dot(vgt[give_half].reshape(rows), nrm[c])
        total = total + dot(vgt_in[give_half].reshape(rows), nrm_in[c])
        ssend[c] = total.astype(BF16).reshape(2, out_rows, LANES)

        @pl.when(i < blocks - tail)
        def _():
            copy_cross(c).start()

        @pl.when(i >= blocks - tail)
        def _():
            copy_far(c).start()

    def give_rows(i, slot):
        c = column_at(i)
        total = dot(vgt[give_half, slot], nrm[c])
        total = total + dot(vgt_in[give_half, slot], nrm_in[c])
        ssend[c, slot] = total.astype(BF16)

    def theirs(i):
        c = column_at(i)
        total = dot(vgt[keep_half].reshape(2 * out_rows, tokens), nrm[c])
        kept[c] = total.reshape(2, out_rows, LANES)
        halves = jnp.logical_or(
            i >= blocks - tail, jnp.logical_and(sec == 0, i < 2)
        )

        @pl.when(jnp.logical_not(halves))
        def _():
            copy_cross(c).wait_recv()

        @pl.when(halves)
        def _():
            wait_far(c)

        @pl.when(jnp.logical_and(sec == 0, i < 2))
        def _():
            wait_near(i)

        total = kept[c, mate_slot] + srecv[c, mate_slot].astype(F32)
        rt[0, c] = total.astype(BF16)
        copy_wg(c).start()

    def mine(i, near=False):
        c = column_at(i)
        total = kept[c, own_slot] + dot(vgt_in[keep_half, own_slot], nrm_in[c])
        if near:
            wait_near(i)
        total = total + srecv[c, own_slot].astype(F32)
        wg_ref[:, lanes(c * LANES)] = total.astype(BF16)

    acc[...] = jnp.zeros_like(acc)

    def part_step(s, carry):
        kk = 3 - s // chunks
        chunk = lax.rem(s, chunks)
        rows = row_chunk(chunk)
        q = peer(kk)

        part = jnp.dot(vg_v[rows], w_v[kk], preferred_element_type=F32).astype(BF16)
        psend[kk, rows] = part
        first = jnp.zeros((ROWS, LANES), F32)
        second = jnp.zeros((ROWS, LANES), F32)
        mean = mean_v[rows]
        inv = inv_v[rows]
        for j in range(per_quarter):
            cols = lanes(q * quarter + j * LANES)
            local = part[:, j * LANES : (j + 1) * LANES].astype(F32) * gain_ref[:, cols]
            white = (st_v[rows, cols].astype(F32) - mean) * inv
            first = first + local
            second = second + local * white
        acc[0, rows] += first
        acc[1, rows] += second

        direct = jnp.logical_or(kk == 3, kk == 1 + chunk // upper)

        ready = jnp.logical_or(outer, jnp.logical_and(sec == 1, kk == 3))

        @pl.when(jnp.logical_and(direct, ready))
        def _():
            copy_part(kk, chunk).start()

        return carry

    pltpu.make_async_copy(w_v, w_v, load_sem.at[2]).wait()
    lax.fori_loop(0, 2 * chunks, part_step, 0)

    @pl.when(hold)
    def _():
        copy_give(own_slot, 0).wait_recv()
        forward(0)
        give_rows(0, own_slot)
        copy_far(column_at(0)).start()
        wait_normed(column_at(1))
        give_rows(1, own_slot)
        copy_far(column_at(1)).start()
        copy_give(mate_slot, 1).wait_recv()
        for i in range(2):
            give_rows(i, mate_slot)
            copy_near(i).start()

    def send_sums():
        lane = lax.broadcasted_iota(jnp.int32, (tokens, LANES), 1)
        sum0 = jnp.sum(acc[0], axis=-1, keepdims=True)
        sum1 = jnp.sum(acc[1], axis=-1, keepdims=True)
        packed = jnp.where(lane == 0, sum0, jnp.where(lane == 1, sum1, 0.0))
        sums[0] = packed.T[:8]
        copy_sums(0).start()

    @pl.when(jnp.logical_or(outer, sec == 1))
    def _():
        lax.fori_loop(2 * chunks, 4 * chunks, part_step, 0)

    @pl.when(jnp.logical_or(outer, sec == 1))
    def _():
        send_sums()

    @pl.when(outer)
    def _():
        pass_all()

    @pl.when(late)
    def _():
        copy_give(mate_slot, 0).start()
        copy_give(own_slot, 1).start()
        send_normed(0, per_quarter)
        copy_keep(mate_slot).start()

    @pl.when(early)
    def _():
        send_normed(3, per_quarter)
        copy_keep(mate_slot).start()

    def copy_above(chunk):
        rows = row_chunk(chunk)
        return remote(
            res_ref.at[rows],
            above_in.at[rows],
            above_send,
            above_recv.at[chunk],
            {"section": 1 - sec},
        )

    def residual():
        load_top.wait()
        copy_sums(1).wait_recv()
        total = sums[1] + sums_in[1]
        total = jnp.concatenate([total] * (LANES // 8), axis=0) * (1.0 / width)
        total = total.T
        acc[0] = jnp.broadcast_to(total[:, 0:1], (tokens, LANES))
        acc[1] = jnp.broadcast_to(total[:, 1:2], (tokens, LANES))

        def rows_step(chunk, carry):
            rows = row_chunk(chunk)
            for kk in (1, 2):
                copy_part(kk, chunk).wait_recv()
            mean = mean_v[rows]
            inv = inv_v[rows]
            for j in range(per_quarter):
                here = slice(j * LANES, (j + 1) * LANES)
                cols = lanes(m * quarter + j * LANES)
                grad = psend[0, rows, here].astype(F32)
                for kk in (1, 2):
                    grad = grad + precv[kk, rows, here].astype(F32)
                scaled = grad * gain_ref[:, cols]
                white = (st_v[rows, cols].astype(F32) - mean) * inv
                branch = inv * (scaled - acc[0, rows] - white * acc[1, rows])
                branch_v[rows, here] = branch
                res_ref[rows, here] = (top_v[rows, here].astype(F32) + branch).astype(
                    BF16
                )

            @pl.when(sec == 1)
            def _():
                copy_above(chunk).start()

            return carry

        lax.fori_loop(0, chunks, rows_step, 0)

    def residual_lower():
        @pl.when(sec == 0)
        def _():
            def lower(chunk, carry):
                rows = row_chunk(chunk)
                copy_above(chunk).wait_recv()
                res_ref[rows] = (above_in[rows].astype(F32) + branch_v[rows]).astype(
                    BF16
                )
                return carry

            lax.fori_loop(0, chunks, lower, 0)

    @pl.when(outer)
    def _():
        pass_sums()
        residual()
        residual_lower()

        def finish(i, carry):
            c = column_at(i)
            own = jnp.dot(vgt[keep_half, own_slot], nrm[c], preferred_element_type=F32)
            copy_wg(c).wait_recv()
            wg_ref[:, lanes(c * LANES)] = (own + rt[1, c].astype(F32)).astype(BF16)
            return carry

        lax.fori_loop(0, blocks, finish, 0)
        copy_give(mate_slot, 0).wait_send()
        copy_give(own_slot, 1).wait_send()
        copy_keep(mate_slot).wait_send()

        several = pl.ds(0, 2 * per_quarter)
        sent(nrm.at[several], nrm_in.at[several], n_send)

    @pl.when(inner)
    def _():
        def step(i):
            give(i)
            following = i // 4 + 1
            soon = jnp.where(sec == 0, following == 2, following >= 3)
            usual = jnp.where(jnp.logical_and(sec == 0, following == 1), 2, 3)
            turn = lax.rem(i, 4) == jnp.where(soon, 1, usual)

            @pl.when(jnp.logical_and(turn, following < per_quarter))
            def _():
                forward(following)

            @pl.when(jnp.logical_and(hold, i == 5))
            def _():
                for chunk in range(0, chunks, 2):
                    copy_part(3, chunk).start()

            @pl.when(jnp.logical_and(hold, i == 9))
            def _():
                for chunk in range(1, chunks, 2):
                    copy_part(3, chunk).start()

            @pl.when(jnp.logical_and(hold, jnp.logical_and(i >= 10, i < 10 + 2 * chunks)))
            def _():
                part_step(i - 10 + 2 * chunks, 0)

            @pl.when(jnp.logical_and(hold, i == 18))
            def _():
                send_sums()

            @pl.when(jnp.logical_and(hold, i == 15))
            def _():
                for chunk in range(0, chunks, 2):
                    copy_part(1 + chunk // upper, chunk).start()

            @pl.when(jnp.logical_and(hold, i == 19))
            def _():
                for chunk in range(1, chunks, 2):
                    copy_part(1 + chunk // upper, chunk).start()

            @pl.when(i >= lag)
            def _():
                theirs(i - lag)

            @pl.when(jnp.logical_and(sec == 1, i == 17))
            def _():
                for chunk in range(chunks):
                    copy_part(1 + chunk // upper, chunk).start()
                pass_sums()
                pass_all()

        @pl.when(sec == 1)
        def _():
            copy_give(own_slot, 0).wait_recv()
            copy_give(mate_slot, 1).wait_recv()
            forward(0)

        def main(i, carry):
            step(i)
            return carry

        lax.fori_loop(2 - 2 * sec, blocks, main, 0)

        def send_near(i, carry):
            copy_near(i).start()
            return carry

        lax.fori_loop(blocks - tail, blocks, send_near, 0)

        @pl.when(sec == 0)
        def _():
            pass_sums()
            pass_all()

        copy_keep(own_slot).wait_recv()

        def last_far(i, carry):
            theirs(i)

            @pl.when(i < blocks - 2)
            def _():
                for k in range(2):
                    mine(2 * (i - (blocks - lag)) + k)

            return carry

        lax.fori_loop(blocks - lag, blocks, last_far, 0)

        @pl.when(sec == 1)
        def _():
            residual()

        def last_near(i, carry):
            mine(i, near=True)
            return carry

        lax.fori_loop(blocks - tail, blocks, last_near, 0)

        @pl.when(sec == 0)
        def _():
            residual()

        residual_lower()

        several = pl.ds(0, 2 * per_quarter)
        sent(ssend, srecv, s_send)
        sent(nrm_in.at[several], nrm_in.at[several], fwd_send)
        sent(rt.at[0], rt.at[1], rt_send)

    three = pl.ds(0, 3)
    for step in range(2):
        copy_sums(step).wait_send()
    sent(psend.at[three], precv.at[three], p_send)

    @pl.when(sec == 1)
    def _():
        sent(res_ref, above_in, above_send)


def fused(value_grad, stream, weights, gain, top_grad, counts):
    tokens, width = stream.shape[1:]
    feats = value_grad.shape[2]
    quarter = width // lax.axis_size("mp")
    out_rows = feats // lax.axis_size("dp")
    blocks = width // LANES
    per_quarter = quarter // LANES
    chunks = tokens // ROWS
    dma = pltpu.SemaphoreType.DMA
    vmem = pltpu.VMEM
    in_hbm = pl.BlockSpec(memory_space=pltpu.HBM)
    in_vmem = pl.BlockSpec(memory_space=pltpu.VMEM)
    placed = [
        pltpu.with_memory_space_constraint(a, pltpu.HBM)
        for a in (value_grad, stream, weights, gain, top_grad)
    ]
    weight_grad, residual_grad = pl.pallas_call(
        functools.partial(kernel, (tokens, width, feats, quarter, out_rows)),
        out_shape=(
            jax.ShapeDtypeStruct((out_rows, width), BF16),
            jax.ShapeDtypeStruct((tokens, quarter), BF16),
        ),
        in_specs=[
            in_hbm,
            in_hbm,
            in_hbm,
            in_hbm,
            in_hbm,
            pl.BlockSpec(memory_space=pltpu.SMEM),
        ],
        out_specs=(in_vmem, in_vmem),
        scratch_shapes=[
            vmem((tokens, feats), BF16),
            vmem((tokens, width), BF16),
            vmem((4, feats, quarter), BF16),
            vmem((tokens, quarter), BF16),
            vmem((1, width), F32),
            vmem((tokens, LANES), F32),
            vmem((tokens, LANES), F32),
            vmem((blocks, tokens, LANES), BF16),
            vmem((blocks, tokens, LANES), BF16),
            vmem((2, 2, out_rows, tokens), BF16),
            vmem((2, 2, out_rows, tokens), BF16),
            vmem((blocks, 2, out_rows, LANES), BF16),
            vmem((blocks, 2, out_rows, LANES), BF16),
            vmem((2, blocks, out_rows, LANES), BF16),
            vmem((blocks, 2, out_rows, LANES), F32),
            vmem((4, tokens, quarter), BF16),
            vmem((4, tokens, quarter), BF16),
            vmem((2, tokens, LANES), F32),
            vmem((2, 8, tokens), F32),
            vmem((2, 8, tokens), F32),
            vmem((tokens, quarter), BF16),
            vmem((tokens, quarter), F32),
            dma((5,)),
            dma,
            dma((blocks,)),
            dma,
            dma((3,)),
            dma((3,)),
            dma,
            dma((blocks,)),
            dma((10,)),
            dma,
            dma,
            dma((3, chunks)),
            dma((2,)),
            dma((2,)),
            dma,
            dma((chunks,)),
        ],
        compiler_params=pltpu.CompilerParams(
            collective_id=0, has_side_effects=True, vmem_limit_bytes=51 * 2**20
        ),
    )(*placed, counts)
    held = [
        pltpu.with_memory_space_constraint(a, pltpu.VMEM)
        for a in (weight_grad, residual_grad)
    ]
    weight_grad, residual_grad = pl.pallas_call(
        store,
        out_shape=tuple(jax.ShapeDtypeStruct(a.shape, a.dtype) for a in held),
        in_specs=[in_vmem, in_vmem],
        out_specs=(in_hbm, in_hbm),
        scratch_shapes=[dma((8,))],
    )(*held)
    return weight_grad[None], residual_grad[None]


def store(weight_ref, residual_ref, weight_out, residual_out, sem):
    copies = []
    for k, (src, dst) in enumerate(((weight_ref, weight_out), (residual_ref, residual_out))):
        share = src.shape[0] // 4
        for h in range(4):
            rows = pl.ds(h * share, share)
            copies.append(pltpu.make_async_copy(src.at[rows], dst.at[rows], sem.at[4 * k + h]))
    for copy in copies:
        copy.start()
    for copy in copies:
        copy.wait()


def normalize(stream_rows):
    values = stream_rows.astype(F32)
    average = jnp.mean(values, axis=-1, keepdims=True)
    centred = values - average
    variance = jnp.mean(centred * centred, axis=-1, keepdims=True)
    inv_scale = lax.rsqrt(variance + EPS)
    return (centred * inv_scale, inv_scale)


def collectives(value_grad, stream, weights, gain, top_grad, counts):
    section_index = lax.axis_index("section")
    model_index = lax.axis_index("mp")
    row_total = stream.shape[1]
    whitened, inv_scale = normalize(stream[0])
    gain_row = gain[0]
    width = whitened.shape[1]
    share = width // lax.axis_size("mp")
    first_col = model_index * share
    cols = lambda a: lax.dynamic_slice_in_dim(a, first_col, share, 1)
    partial = jnp.dot(value_grad[0], weights[0], preferred_element_type=F32)
    partial = partial.astype(BF16)
    local = partial.astype(F32) * gain_row
    sums = jnp.stack([jnp.sum(local, -1), jnp.sum(local * whitened, -1)])
    norm_grad = lax.psum_scatter(partial, "mp", scatter_dimension=1, tiled=True)
    sums = lax.psum(sums, "mp") * (1.0 / width)
    normed = (whitened * gain_row).astype(BF16)
    micro_index = jnp.arange(row_total, dtype=jnp.int32) // TOK_MB
    live_mask = (micro_index < counts[0]).astype(BF16)
    masked = value_grad[0] * live_mask[:, None]
    product = lax.dot_general(
        masked, normed, (((0,), (0,)), ((), ())), preferred_element_type=F32
    )
    weight_grad = lax.psum_scatter(
        product.astype(BF16), "dp", scatter_dimension=0, tiled=True
    )[None]
    scaled = norm_grad.astype(F32) * cols(gain)
    branch = inv_scale * (scaled - sums[0][:, None] - cols(whitened) * sums[1][:, None])
    above = (cols(top_grad).astype(F32) + branch).astype(BF16)
    below = lax.ppermute(above, "section", [(1, 0)])
    lower = (below.astype(F32) + branch).astype(BF16)
    result = jnp.where(section_index == 0, lower, above)
    return (weight_grad, result[None])


def solution(mesh):
    in_specs = (
        P("section", "dp", "mp"),
        P("section", "dp", None),
        P("section", "mp", None),
        P("section", None),
        P("dp", None),
        P("dp"),
    )
    out_specs = (P("section", ("mp", "dp"), None), P("section", "dp", "mp"))
    grid = (mesh.shape["section"], mesh.shape["mp"], mesh.shape["dp"])
    step = fused if grid == (2, 4, 4) else collectives
    return jax.shard_map(step, mesh=mesh, in_specs=in_specs, out_specs=out_specs, check_vma=False)
```
